32 devices in a mesh: section: 8 (over z, x), dp: 4 (over y, core).
Axes of the slice: x: 2, y: 2, z: 4, core: 2. Of those that a mesh axis runs over, the one named last changes fastest.
Arguments:
- carry_act: bfloat16 [8, 32, 2304], P('section', 'dp'), may hold values from -6 to 6
- carry_act_tan: bfloat16 [8, 32, 2304], P('section', 'dp'), may hold values from -6 to 6
- carry_adj: bfloat16 [8, 32, 2304], P('section', 'dp'), may hold values from -0.75 to 0.75
- carry_adj_tan: bfloat16 [8, 32, 2304], P('section', 'dp'), may hold values from -0.75 to 0.75
- fresh_act: bfloat16 [2, 32, 2304], P(None, 'dp'), may hold values from -6 to 6
- loss_cot: bfloat16 [2, 32, 2304], P(None, 'dp'), may hold values from -0.75 to 0.75
- stash_act: bfloat16 [8, 2, 32, 2304], P('section', None, 'dp'), may hold values from -6 to 6
- stash_act_tan: bfloat16 [8, 2, 32, 2304], P('section', None, 'dp'), may hold values from -6 to 6
- norm_gain: bfloat16 [8, 2304], P('section'), may hold values from 0.25 to 1.75
- up_weight: bfloat16 [8, 2304, 4608], P('section', None, 'dp'), may hold values from -0.125 to 0.125
- down_weight: bfloat16 [8, 4608, 2304], P('section', 'dp'), may hold values from -0.09375 to 0.09375
- up_dir: bfloat16 [8, 2304, 4608], P('section', None, 'dp'), may hold values from -0.125 to 0.125
- down_dir: bfloat16 [8, 4608, 2304], P('section', 'dp'), may hold values from -0.09375 to 0.09375
Outputs:
- next_act: bfloat16 [8, 32, 2304], P('section', 'dp')
- next_act_tan: bfloat16 [8, 32, 2304], P('section', 'dp')
- next_adj: bfloat16 [8, 32, 2304], P('section', 'dp')
- next_adj_tan: bfloat16 [8, 32, 2304], P('section', 'dp')
- hvp_up: bfloat16 [8, 2304, 4608], P('section', None, 'dp')
- hvp_down: bfloat16 [8, 4608, 2304], P('section', 'dp')
The draws below stay inside these ranges and needn't reach their ends.
All inputs are finite; a program needn't handle non-finite values.
Results may differ from the reference program's by a relative error of at most 0.02.
Values may be sent and summed in bfloat16 or wider, within the bound.
A program may use at most 128 MiB of HBM per device.

```python
import jax
import jax.numpy as jnp
from jax import lax

D = 2304
FF = 4608
TICKS = 2
TOKENS = 32
SECTIONS = 8
N_DP = 4


def block_levels(key, dims, split, low, top_value):
    factor_of = 1.0
    for position, blocks in split:
        draws = jax.random.uniform(jax.random.fold_in(jax.random.fold_in(key, 6), position), (blocks,), jnp.float32, low / len(split), top_value / len(split))
        factor_of = factor_of * jnp.repeat(jnp.exp(draws), dims[position] // blocks).reshape((-1,) + (1,) * (len(dims) - 1 - position))
    return factor_of


def noise(own_key, dims, scale, reach, cuts=(), dtype=jnp.bfloat16):
    entries = scale * jax.random.normal(own_key, dims, jnp.float32)
    if cuts:
        entries = entries * block_levels(own_key, dims, cuts, -0.22, 0.18)
    return jnp.clip(entries, -reach, reach).astype(dtype)


def setup_inputs(seed: int = 0) -> dict:
    splits = jax.random.split(jax.random.key(seed), 14)
    carry_act = noise(splits[0], (SECTIONS, TOKENS, D), 1.0, 6.0, ((0, 8), (1, 4)))
    carry_act_tan = noise(splits[1], (SECTIONS, TOKENS, D), 1.0, 6.0, ((0, 8), (1, 4)))
    carry_adj = noise(splits[2], (SECTIONS, TOKENS, D), 0.125, 0.75, ((0, 8), (1, 4)))
    carry_adj_tan = noise(splits[3], (SECTIONS, TOKENS, D), 0.125, 0.75, ((0, 8), (1, 4)))
    fresh_act = noise(splits[4], (TICKS, TOKENS, D), 1.0, 6.0, ((1, 4),))
    loss_cot = noise(splits[5], (TICKS, TOKENS, D), 0.125, 0.75, ((1, 4),))
    stash_act = noise(splits[6], (SECTIONS, TICKS, TOKENS, D), 1.0, 6.0, ((0, 8), (2, 4)))
    stash_act_tan = noise(splits[7], (SECTIONS, TICKS, TOKENS, D), 1.0, 6.0, ((0, 8), (2, 4)))
    norm_gain = jnp.clip(1.0 + 0.15 * jax.random.normal(splits[8], (SECTIONS, D), jnp.float32), 0.25, 1.75).astype(jnp.bfloat16)
    up_weight = noise(splits[9], (SECTIONS, D, FF), D ** -0.5, 0.125, ((0, 8), (2, 4)))
    down_weight = noise(splits[10], (SECTIONS, FF, D), FF ** -0.5, 0.09375, ((0, 8), (1, 4)))
    up_dir = noise(splits[11], (SECTIONS, D, FF), D ** -0.5, 0.125, ((0, 8), (2, 4)))
    down_dir = noise(splits[12], (SECTIONS, FF, D), FF ** -0.5, 0.09375, ((0, 8), (1, 4)))
    return dict(carry_act=carry_act, carry_act_tan=carry_act_tan, carry_adj=carry_adj, carry_adj_tan=carry_adj_tan, fresh_act=fresh_act, loss_cot=loss_cot, stash_act=stash_act, stash_act_tan=stash_act_tan, norm_gain=norm_gain, up_weight=up_weight, down_weight=down_weight, up_dir=up_dir, down_dir=down_dir)


sqrt_two_over_pi = 0.7978845608028654
cubic_coef = 0.044715
norm_eps = 1e-06

def gelu_parts(linear):
    inner_arg = sqrt_two_over_pi * (linear + cubic_coef * linear * linear * linear)
    first_slope = sqrt_two_over_pi * (1.0 + 3.0 * cubic_coef * linear * linear)
    second_slope = 6.0 * sqrt_two_over_pi * cubic_coef * linear
    tanh_value = jnp.tanh(inner_arg)
    sech_square = 1.0 - tanh_value * tanh_value
    gelu_value = 0.5 * linear * (1.0 + tanh_value)
    gelu_first = 0.5 * (1.0 + tanh_value) + 0.5 * linear * sech_square * first_slope
    gelu_second = sech_square * (first_slope - linear * tanh_value * first_slope * first_slope + 0.5 * linear * second_slope)
    return (gelu_value, gelu_first, gelu_second)

def matrix_product(left, right):
    return jnp.dot(left, right, preferred_element_type=jnp.float32)

def product_last(left, right):
    return lax.dot_general(left, right, (((1,), (1,)), ((), ())), preferred_element_type=jnp.float32)

def product_first(left, right):
    return lax.dot_general(left, right, (((0,), (0,)), ((), ())), preferred_element_type=jnp.float32)

def norm_stats(rows, rows_tan):
    values = rows.astype(jnp.float32)
    values_tan = rows_tan.astype(jnp.float32)
    inverse = lax.rsqrt(lax.optimization_barrier(jnp.mean(values * values, axis=-1, keepdims=True)) + norm_eps)
    inverse_tan = -(inverse * inverse * inverse) * lax.optimization_barrier(jnp.mean(values * values_tan, axis=-1, keepdims=True))
    return (values, values_tan, inverse, inverse_tan)

def norm_rows(rows, rows_tan, gain_row):
    values, values_tan, inverse, inverse_tan = norm_stats(rows, rows_tan)
    gain_wide = gain_row.astype(jnp.float32)
    normed = (values * inverse * gain_wide).astype(jnp.bfloat16)
    normed_tan = ((values_tan * inverse + values * inverse_tan) * gain_wide).astype(jnp.bfloat16)
    return (normed, normed_tan)

def norm_back(rows, rows_tan, gain_row, arriving, arriving_tan, summed, summed_tan):
    values, values_tan, inverse, inverse_tan = norm_stats(rows, rows_tan)
    gain_wide = gain_row.astype(jnp.float32)
    weighted = summed * gain_wide
    weighted_tan = summed_tan * gain_wide
    moment = lax.optimization_barrier(jnp.mean(values * weighted, axis=-1, keepdims=True))
    moment_tan = lax.optimization_barrier(jnp.mean(values_tan * weighted + values * weighted_tan, axis=-1, keepdims=True))
    inverse_cube = inverse * inverse * inverse
    returned = arriving.astype(jnp.float32) + inverse * weighted - inverse_cube * values * moment
    returned_tan = arriving_tan.astype(jnp.float32) + inverse_tan * weighted + inverse * weighted_tan - 3.0 * inverse * inverse * inverse_tan * values * moment - inverse_cube * values_tan * moment - inverse_cube * values * moment_tan
    return (returned.astype(jnp.bfloat16), returned_tan.astype(jnp.bfloat16))

def branch_forward(normed, normed_tan, up_local, down_local, up_direction, down_direction):
    linear = matrix_product(normed, up_local)
    linear_tan = matrix_product(normed_tan, up_local) + matrix_product(normed, up_direction)
    gelu_value, gelu_first, gelu_second = gelu_parts(linear)
    hidden = gelu_value.astype(jnp.bfloat16)
    hidden_tan = (gelu_first * linear_tan).astype(jnp.bfloat16)
    partial_value = matrix_product(hidden, down_local)
    partial_tan = matrix_product(hidden_tan, down_local) + matrix_product(hidden, down_direction)
    return (partial_value, partial_tan)

def branch_backward(stash_normed, stash_normed_tan, adjoint_all, adjoint_all_tan, up_local, down_local, up_direction, down_direction):
    linear = matrix_product(stash_normed, up_local)
    linear_tan = matrix_product(stash_normed_tan, up_local) + matrix_product(stash_normed, up_direction)
    gelu_value, gelu_first, gelu_second = gelu_parts(linear)
    hidden = gelu_value.astype(jnp.bfloat16)
    hidden_tan = (gelu_first * linear_tan).astype(jnp.bfloat16)
    upstream = product_last(adjoint_all, down_local)
    upstream_tan = product_last(adjoint_all_tan, down_local) + product_last(adjoint_all, down_direction)
    deltas = (upstream * gelu_first).astype(jnp.bfloat16)
    deltas_tan = (upstream_tan * gelu_first + upstream * gelu_second * linear_tan).astype(jnp.bfloat16)
    curvature_down = product_first(hidden_tan, adjoint_all) + product_first(hidden, adjoint_all_tan)
    curvature_up = product_first(stash_normed_tan, deltas) + product_first(stash_normed, deltas_tan)
    partial_value = product_last(deltas, up_local)
    partial_tan = product_last(deltas_tan, up_local) + product_last(deltas, up_direction)
    return (partial_value, partial_tan, curvature_up, curvature_down)

def sum_slices(parts):
    rounded = lax.optimization_barrier(parts.astype(jnp.bfloat16)).astype(jnp.float32)
    return lax.optimization_barrier(jnp.sum(rounded, axis=0))

def one_section(packed):
    input_rows, input_tan, arriving, arriving_tan, stash_rows, stash_tan, gain_row, up_section, down_section, up_section_dir, down_section_dir = packed
    width = FF // N_DP
    up_sliced = jnp.moveaxis(up_section.reshape(D, N_DP, width), 1, 0)
    up_dir_sliced = jnp.moveaxis(up_section_dir.reshape(D, N_DP, width), 1, 0)
    down_sliced = down_section.reshape(N_DP, width, D)
    down_dir_sliced = down_section_dir.reshape(N_DP, width, D)
    normed, normed_tan = norm_rows(input_rows, input_tan, gain_row)

    def forward_slice(weights):
        return branch_forward(normed, normed_tan, weights[0], weights[1], weights[2], weights[3])
    partials = lax.map(forward_slice, (up_sliced, down_sliced, up_dir_sliced, down_dir_sliced))
    new_act = (input_rows.astype(jnp.float32) + sum_slices(partials[0])).astype(jnp.bfloat16)
    new_act_tan = (input_tan.astype(jnp.float32) + sum_slices(partials[1])).astype(jnp.bfloat16)
    stash_normed, stash_normed_tan = norm_rows(stash_rows, stash_tan, gain_row)

    def backward_slice(weights):
        return branch_backward(stash_normed, stash_normed_tan, arriving, arriving_tan, weights[0], weights[1], weights[2], weights[3])
    backs = lax.map(backward_slice, (up_sliced, down_sliced, up_dir_sliced, down_dir_sliced))
    summed = sum_slices(backs[0])
    summed_tan = sum_slices(backs[1])
    curvature_up = jnp.moveaxis(backs[2], 0, 1).reshape(D, FF)
    curvature_down = backs[3].reshape(FF, D)
    new_adj, new_adj_tan = norm_back(stash_rows, stash_tan, gain_row, arriving, arriving_tan, summed, summed_tan)
    return (new_act, new_act_tan, new_adj, new_adj_tan, curvature_up, curvature_down)

def reference(carry_act, carry_act_tan, carry_adj, carry_adj_tan, fresh_act, loss_cot, stash_act, stash_act_tan, norm_gain, up_weight, down_weight, up_dir, down_dir):
    activation, activation_tan = (carry_act, carry_act_tan)
    adjoint, adjoint_tan = (carry_adj, carry_adj_tan)
    total_up = jnp.zeros(up_weight.shape, jnp.float32)
    total_down = jnp.zeros(down_weight.shape, jnp.float32)
    for tick_index in range(TICKS):
        zero_rows = jnp.zeros_like(fresh_act[tick_index])
        input_rows = jnp.concatenate([fresh_act[tick_index][None], activation[:-1]], axis=0)
        input_tan = jnp.concatenate([zero_rows[None], activation_tan[:-1]], axis=0)
        arriving = jnp.concatenate([adjoint[1:], loss_cot[tick_index][None]], axis=0)
        arriving_tan = jnp.concatenate([adjoint_tan[1:], zero_rows[None]], axis=0)
        results = lax.map(one_section, (input_rows, input_tan, arriving, arriving_tan, stash_act[:, tick_index], stash_act_tan[:, tick_index], norm_gain, up_weight, down_weight, up_dir, down_dir))
        activation, activation_tan, adjoint, adjoint_tan = (results[0], results[1], results[2], results[3])
        total_up = total_up + results[4]
        total_down = total_down + results[5]
    return (activation, activation_tan, adjoint, adjoint_tan, total_up.astype(jnp.bfloat16), total_down.astype(jnp.bfloat16))
```

```python
import functools

import jax
import jax.numpy as jnp
from jax import lax
from jax.experimental import pallas as pl
from jax.experimental.pallas import tpu as pltpu
from jax.sharding import PartitionSpec as P

sqrt_two_over_pi = 0.7978845608028654
cubic_coef = 0.044715
norm_eps = 1e-06


def gelu_parts(linear):
    inner_arg = sqrt_two_over_pi * (linear + cubic_coef * linear * linear * linear)
    first_slope = sqrt_two_over_pi * (1.0 + 3.0 * cubic_coef * linear * linear)
    second_slope = 6.0 * sqrt_two_over_pi * cubic_coef * linear
    tanh_value = jnp.tanh(inner_arg)
    sech_square = 1.0 - tanh_value * tanh_value
    gelu_value = 0.5 * linear * (1.0 + tanh_value)
    gelu_first = 0.5 * (1.0 + tanh_value) + 0.5 * linear * sech_square * first_slope
    gelu_second = sech_square * (
        first_slope - linear * tanh_value * first_slope * first_slope + 0.5 * linear * second_slope
    )
    return (gelu_value, gelu_first, gelu_second)


def matrix_product(left, right):
    return jnp.dot(left, right, preferred_element_type=jnp.float32)


def product_last(left, right):
    return lax.dot_general(
        left, right, (((1,), (1,)), ((), ())), preferred_element_type=jnp.float32
    )


def product_first(left, right):
    return lax.dot_general(
        left, right, (((0,), (0,)), ((), ())), preferred_element_type=jnp.float32
    )


f32, bf16 = (jnp.float32, jnp.bfloat16)
MESH = pl.DeviceIdType.MESH


def lane_chunk(size, wanted):
    fits = [c for c in range(128, wanted + 1, 128) if size % c == 0]
    return max(fits) if fits else size


def over_chunks(size, chunk, body, after=None):
    for index in range(size // chunk):
        body(pl.ds(index * chunk, chunk))
        if after is not None:
            after(index)


def turn(source, target, chunk):
    def step(index, carry):
        where = pl.ds(pl.multiple_of(index * chunk, chunk), chunk)
        target[:, where] = source[where, :].T
        return carry

    lax.fori_loop(0, source.shape[0] // chunk, step, 0)


def pair(value, tangent):
    blocks, rows, width = value.shape
    return jnp.stack([value, tangent], axis=1).reshape(blocks * 2 * rows, width)


def unpair(stacked, rows):
    wide = stacked.astype(f32).reshape(-1, 2, rows, stacked.shape[-1])
    return (wide[:, 0], wide[:, 1])


def norm_pair(stacked, gain, rows):
    values, values_tan = unpair(stacked, rows)
    inverse = lax.rsqrt(jnp.mean(values * values, axis=-1, keepdims=True) + norm_eps)
    inverse_tan = -(inverse * inverse * inverse) * jnp.mean(
        values * values_tan, axis=-1, keepdims=True
    )
    return (values * inverse * gain, (values_tan * inverse + values * inverse_tan) * gain)


def relay_kernel(
    sections, n_dp, ticks,
    carry_act, carry_act_tan, carry_adj, carry_adj_tan, fresh_act, loss_cot, stash_act,
    stash_act_tan, norm_gain, up_hbm, down_hbm, up_dir_hbm, down_dir_hbm,
    stash_out, adj_out, hidden_out, delta_out, final_out,
    up, down, up_dir, down_dir, up_turned, down_turned, up_dir_turned, down_dir_turned,
    gain_row, own_stash,
    left, left_dir, hid, hid_dir, slope, bend, hid_swap, delta, delta_dir, delta_swap,
    adj_dir, stash_all, gathered, outgoing, partial, from_core, to_chip, from_chip,
    weight_sems, small_sems, edge_loads, out_sems, core_sems, chip_sems, shift_sems, edge_sems,
    relay_sems, stash_sems, stash_relay,
):
    chips = n_dp // 2
    rows = carry_act.shape[1]
    width = carry_act.shape[2]
    units = up.shape[1]
    band = n_dp * 2 * rows
    unit_chunk = lane_chunk(units, 384)
    width_chunk = lane_chunk(width, 768)
    pieces = width // width_chunk
    section, part = (lax.axis_index("section"), lax.axis_index("dp"))
    chip, core = (part // 2, part % 2)
    other = 1 - core
    partner = (section, chip * 2 + other)
    first, last_one = (section == 0, section == sections - 1)
    inner_first, inner_last = (section > 0, section < sections - 1)
    turned = units % 128 == 0

    def chip_at(step):
        return lax.rem(chip + step, chips)

    def load_pair(index, value, tangent, target):
        return [
            pltpu.make_async_copy(value, target.at[pl.ds(0, rows)], small_sems.at[index, 0]),
            pltpu.make_async_copy(tangent, target.at[pl.ds(rows, rows)], small_sems.at[index, 1]),
        ]

    stash_loads = [
        load_pair(t, stash_act.at[0, t], stash_act_tan.at[0, t], own_stash.at[t])
        for t in range(ticks)
    ]
    adj_loads = load_pair(ticks, carry_adj.at[0], carry_adj_tan.at[0], outgoing.at[1])
    act_loads = load_pair(ticks + 1, carry_act.at[0], carry_act_tan.at[0], outgoing.at[0])
    gain_load = pltpu.make_async_copy(norm_gain, gain_row, small_sems.at[ticks + 2, 0])

    def edge_load(lane):
        source = (fresh_act, loss_cot)[lane % 2]
        return pltpu.make_async_copy(
            source.at[lane // 2],
            gathered.at[lane, core, chip, pl.ds(0, rows)],
            edge_loads.at[lane],
        )

    def at_edge(lane):
        return first if lane % 2 == 0 else last_one

    def inside(lane):
        return inner_first if lane % 2 == 0 else inner_last

    def sends(lane):
        return inner_last if lane % 2 == 0 else inner_first

    def call(work, *given):
        return functools.partial(work, *given)

    def start_all(copies):
        for copy in copies:
            copy.start()

    def wait_all(copies):
        for copy in copies:
            copy.wait()

    gain_load.start()
    for tick in range(ticks):
        start_all(stash_loads[tick])
    start_all(adj_loads)
    start_all(act_loads)
    for lane in range(2 * ticks):
        pl.when(at_edge(lane))(edge_load(lane).start)

    def weight_loads(number, source, target):
        cuts = weight_sems.shape[1]
        part = target.shape[0] // cuts
        return [
            pltpu.make_async_copy(
                source.at[0, pl.ds(cut * part, part)],
                target.at[pl.ds(cut * part, part)],
                weight_sems.at[number, cut],
            )
            for cut in range(cuts)
        ]

    loads = [
        weight_loads(i, source, target)
        for i, (source, target) in enumerate(
            ((up_hbm, up), (up_dir_hbm, up_dir), (down_hbm, down), (down_dir_hbm, down_dir))
        )
    ]

    barrier = pltpu.get_barrier_semaphore()

    def greet(where, place):
        pl.semaphore_signal(barrier, inc=1, device_id=(where, place), device_id_type=MESH)

    def greet_section(where):
        for step in range(chips):
            greet(where, chip_at(step) * 2 + core)

    pl.when(inner_last)(lambda: greet_section(section + 1))
    pl.when(inner_first)(lambda: greet_section(section - 1))
    pl.semaphore_signal(barrier, inc=1, device_id=partner, device_id_type=MESH)
    for step in range(1, chips):
        greet(section, chip_at(step) * 2 + core)

    def columns(piece):
        if isinstance(piece, int):
            return pl.ds(piece * width_chunk, width_chunk)
        return pl.ds(pl.multiple_of(piece * width_chunk, width_chunk), width_chunk)

    def shift_copies(lane, piece):
        where = section + 1 if lane % 2 == 0 else section - 1
        cols = columns(piece)
        return [
            pltpu.make_async_remote_copy(
                src_ref=outgoing.at[lane, :, cols],
                dst_ref=gathered.at[lane, core, chip, :, cols],
                send_sem=shift_sems.at[lane, piece, 0, step],
                recv_sem=shift_sems.at[lane, piece, 1, step],
                device_id=(where, chip_at(step) * 2 + core),
                device_id_type=MESH,
            )
            for step in range(chips)
        ]

    def edge_copies(lane):
        return [
            pltpu.make_async_remote_copy(
                src_ref=gathered.at[lane, core, chip],
                dst_ref=gathered.at[lane, core, chip],
                send_sem=edge_sems.at[lane, 0, step],
                recv_sem=edge_sems.at[lane, 1, step],
                device_id=(section, chip_at(step) * 2 + core),
                device_id_type=MESH,
            )
            for step in range(1, chips)
        ]

    def relay_copy(lane, piece):
        cols = columns(piece)
        return pltpu.make_async_remote_copy(
            src_ref=gathered.at[lane, core, :, :, cols],
            dst_ref=gathered.at[lane, core, :, :, cols],
            send_sem=relay_sems.at[lane, piece, 0],
            recv_sem=relay_sems.at[lane, piece, 1],
            device_id=partner,
            device_id_type=MESH,
        )

    def stash_copies(tick):
        return [
            pltpu.make_async_remote_copy(
                src_ref=stash_all.at[tick, core, chip],
                dst_ref=stash_all.at[tick, core, chip],
                send_sem=stash_sems.at[tick, 0, step],
                recv_sem=stash_sems.at[tick, 1, step],
                device_id=(section, chip_at(step) * 2 + core),
                device_id_type=MESH,
            )
            for step in range(1, chips)
        ]

    def stash_relay_copy(tick):
        return pltpu.make_async_remote_copy(
            src_ref=stash_all.at[tick, core],
            dst_ref=stash_all.at[tick, core],
            send_sem=stash_relay.at[tick, 0],
            recv_sem=stash_relay.at[tick, 1],
            device_id=partner,
            device_id_type=MESH,
        )

    def relay_stash(tick):
        for copy in stash_copies(tick):
            copy.wait_recv()
        stash_relay_copy(tick).start()

    def core_copy(lane, piece):
        return pltpu.make_async_remote_copy(
            src_ref=partial.at[lane, other, :, :, columns(piece)],
            dst_ref=from_core.at[lane, :, :, columns(piece)],
            send_sem=core_sems.at[lane, piece, 0],
            recv_sem=core_sems.at[lane, piece, 1],
            device_id=partner,
            device_id_type=MESH,
        )

    def chip_copies(lane, piece):
        return [
            pltpu.make_async_remote_copy(
                src_ref=to_chip.at[lane, step - 1, :, columns(piece)],
                dst_ref=from_chip.at[lane, step - 1, :, columns(piece)],
                send_sem=chip_sems.at[lane, piece, 0, step - 1],
                recv_sem=chip_sems.at[lane, piece, 1, step - 1],
                device_id=(section, chip_at(step) * 2 + core),
                device_id_type=MESH,
            )
            for step in range(1, chips)
        ]

    def shift(lane, piece):
        pl.when(sends(lane))(lambda: start_all(shift_copies(lane, piece)))

    def relay(lane, piece):
        def from_section():
            for copy in shift_copies(lane, piece):
                copy.wait_recv()

        def from_edge():
            for copy in edge_copies(lane):
                copy.wait_recv()

        pl.when(inside(lane))(from_section)
        if piece == 0:
            pl.when(at_edge(lane))(from_edge)
        relay_copy(lane, piece).start()

    def reduce_in_chip(lane, piece):
        core_copy(lane, piece).wait_recv()
        cols = columns(piece)
        for step in range(1, chips):
            place = chip_at(step)
            summed = partial[lane, core, place, :, cols].astype(f32)
            summed = summed + from_core[lane, place, :, cols].astype(f32)
            to_chip[lane, step - 1, :, cols] = summed.astype(bf16)
        start_all(chip_copies(lane, piece))

    def reduced(lane, piece):
        for copy in chip_copies(lane, piece):
            copy.wait_recv()
        cols = columns(piece)
        total = partial[lane, core, chip, :, cols].astype(f32)
        total = total + from_core[lane, chip, :, cols].astype(f32)
        for step in range(chips - 1):
            total = total + from_chip[lane, step, :, cols].astype(f32)
        return total

    def norm_stash(tick):
        gain = gain_row[...].astype(f32)
        normed, normed_tan = norm_pair(own_stash[tick], gain, rows)
        stash_all[tick, core, chip] = pair(normed, normed_tan).astype(bf16)

    outs = []

    def send_out(source, target):
        copy = pltpu.make_async_copy(source, target, out_sems.at[len(outs)])
        copy.start()
        outs.append(copy)

    def stage_forward(tick):
        lane = 2 * tick
        for piece in range(pieces):
            relay_copy(lane, piece).wait_recv()
        gain = gain_row[...].astype(f32)
        for block in range(n_dp):
            where = pl.ds(block * 2 * rows, 2 * rows)
            normed, normed_tan = norm_pair(
                gathered[lane, block // chips, block % chips], gain, rows
            )
            left[where, :] = pair(normed, normed_tan).astype(bf16)
            left_dir[where, :] = pair(jnp.zeros_like(normed), normed).astype(bf16)

    def stage_stash(tick):
        stash_relay_copy(tick).wait_recv()
        for block in range(n_dp):
            where = pl.ds(band + block * 2 * rows, 2 * rows)
            stacked = stash_all[tick, block // chips, block % chips]
            left[where, :] = stacked
            value = unpair(stacked, rows)[0]
            left_dir[where, :] = pair(jnp.zeros_like(value), value).astype(bf16)
        send_out(stash_all.at[tick], stash_out.at[tick])

    def forward_products(cols):
        stacked = matrix_product(left[:band, :], up[:, cols]) + matrix_product(
            left_dir[:band, :], up_dir[:, cols]
        )
        linear, linear_tan = unpair(stacked, rows)
        value, slope_now, _ = gelu_parts(linear)
        hid[:, cols] = pair(value, slope_now * linear_tan).astype(bf16)
        hid_dir[:, cols] = pair(jnp.zeros_like(value), value).astype(bf16)

    def stash_products(tick, cols):
        stacked = matrix_product(left[band:, :], up[:, cols]) + matrix_product(
            left_dir[band:, :], up_dir[:, cols]
        )
        linear, linear_tan = unpair(stacked, rows)
        value, slope_now, second = gelu_parts(linear)
        hid_swap[tick, :, cols] = pair(slope_now * linear_tan, value).astype(bf16)
        slope[tick, :, :, cols] = slope_now
        bend[tick, :, :, cols] = second * linear_tan

    def down_products(lane, cols):
        stacked = matrix_product(hid[...], down[:, cols]) + matrix_product(
            hid_dir[...], down_dir[:, cols]
        )
        partial[lane, :, :, :, cols] = stacked.astype(bf16).reshape(2, chips, 2 * rows, -1)

    def adjoint_products(tick, cols):
        adjoint = gathered[2 * tick + 1].reshape(band, width)
        if turned and tick:
            stacked = matrix_product(adjoint, down_turned[:, cols]) + matrix_product(
                adj_dir[...], down_dir_turned[:, cols]
            )
        elif turned:
            stacked = matrix_product(adjoint, down_turned[:, cols]) + product_last(
                adj_dir[...], down_dir[cols, :]
            )
        else:
            stacked = product_last(adjoint, down[cols, :]) + product_last(
                adj_dir[...], down_dir[cols, :]
            )
        upstream, upstream_tan = unpair(stacked, rows)
        slope_now, second_tan = (slope[tick, :, :, cols], bend[tick, :, :, cols])
        value = upstream * slope_now
        tangent = upstream_tan * slope_now + upstream * second_tan
        delta[:, cols] = pair(value, tangent).astype(bf16)
        delta_dir[:, cols] = pair(jnp.zeros_like(value), value).astype(bf16)
        delta_swap[tick, :, cols] = pair(tangent, value).astype(bf16)

    def back_products(lane, cols):
        if turned:
            stacked = matrix_product(delta[...], up_turned[:, cols]) + matrix_product(
                delta_dir[...], up_dir_turned[:, cols]
            )
        else:
            stacked = product_last(delta[...], up[cols, :]) + product_last(
                delta_dir[...], up_dir[cols, :]
            )
        partial[lane, :, :, :, cols] = stacked.astype(bf16).reshape(2, chips, 2 * rows, -1)

    def finish_forward(tick):
        lane = 2 * tick
        for piece in range(pieces):
            cols = columns(piece)
            total = reduced(lane, piece) + gathered[lane, core, chip, :, cols].astype(f32)
            if tick + 1 < ticks:
                outgoing[lane + 2, :, cols] = total.astype(bf16)
                shift(lane + 2, piece)
            else:
                final_out[0, :, cols] = total[:rows].astype(bf16)
                final_out[1, :, cols] = total[rows:].astype(bf16)

    def finish_backward(tick):
        lane = 2 * tick + 1
        total = jnp.concatenate([reduced(lane, piece) for piece in range(pieces)], axis=-1)
        summed, summed_tan = (total[:rows], total[rows:])
        gain = gain_row[...].astype(f32)
        arriving = gathered[lane, core, chip].astype(f32)
        both = own_stash[tick].astype(f32)
        values, values_tan = (both[:rows], both[rows:])
        inverse = lax.rsqrt(jnp.mean(values * values, axis=-1, keepdims=True) + norm_eps)
        cube = inverse * inverse * inverse
        inverse_tan = -cube * jnp.mean(values * values_tan, axis=-1, keepdims=True)
        weighted, weighted_tan = (summed * gain, summed_tan * gain)
        moment = jnp.mean(values * weighted, axis=-1, keepdims=True)
        moment_tan = jnp.mean(
            values_tan * weighted + values * weighted_tan, axis=-1, keepdims=True
        )
        value = arriving[:rows] + inverse * weighted - cube * values * moment
        tangent = (
            arriving[rows:]
            + inverse_tan * weighted
            + inverse * weighted_tan
            - 3.0 * inverse * inverse * inverse_tan * values * moment
            - cube * values_tan * moment
            - cube * values * moment_tan
        )
        if tick + 1 < ticks:
            outgoing[lane + 2] = pair(value[None], tangent[None]).astype(bf16)
            for piece in range(pieces):
                shift(lane + 2, piece)
        else:
            final_out[2] = value.astype(bf16)
            final_out[3] = tangent.astype(bf16)

    def start_piece(lane, piece):
        core_copy(lane, piece).start()

    def stage_adjoint(tick):
        lane = 2 * tick + 1
        for piece in range(pieces):
            relay_copy(lane, piece).wait_recv()
        for block in range(n_dp):
            value = unpair(gathered[lane, block // chips, block % chips], rows)[0]
            adj_dir[pl.ds(block * 2 * rows, 2 * rows), :] = pair(
                jnp.zeros_like(value), value
            ).astype(bf16)
        send_out(gathered.at[lane], adj_out.at[tick])

    def enter_edge(lane):
        def load_rows():
            edge_load(lane).wait()
            gathered[lane, core, chip, rows:, :] = jnp.zeros((rows, width), bf16)

        pl.when(at_edge(lane))(load_rows)

    def send_edge(lane):
        pl.when(at_edge(lane))(lambda: start_all(edge_copies(lane)))

    gain_load.wait()
    for tick in range(ticks):
        wait_all(stash_loads[tick])
    wait_all(adj_loads)
    wait_all(act_loads)
    for lane in range(2 * ticks):
        enter_edge(lane)
    for load in loads:
        start_all(load)
    norm_stash(0)
    sides = inner_first.astype(jnp.int32) + inner_last.astype(jnp.int32)
    pl.semaphore_wait(barrier, chips + chips * sides)
    start_all(stash_copies(0))

    def first_shift(lane):
        copies = [shift_copies(lane, piece) for piece in range(pieces)]
        for step in range(chips):
            for piece in range(pieces):
                copies[piece][step].start()

    pl.when(sends(1))(call(first_shift, 1))
    pl.when(sends(0))(call(first_shift, 0))
    for lane in (1, 0):
        send_edge(lane)
    for tick in range(1, ticks):
        norm_stash(tick)

    def turn_part(source, target, index):
        where = pl.ds(index * unit_chunk, unit_chunk)
        target[:, where] = source[where, :].T

    def all_pieces(work, *given):
        for piece in range(pieces):
            work(*given, piece)

    def enter_weights(number, source, target):
        part = source.shape[0] // len(loads[number])
        for cut, load in enumerate(loads[number]):
            load.wait()
            if turned:
                where = pl.ds(cut * part, part)
                target[:, where] = source[where, :].T

    enter_weights(0, up, up_turned)
    relay_stash(0)
    enter_weights(1, up_dir, up_dir_turned)
    stage_stash(0)
    wait_all(loads[2])

    def beside_stash(index):
        if turned:
            turn_part(down, down_turned, index)

    over_chunks(units, unit_chunk, call(stash_products, 0), beside_stash)
    send_out(hid_swap.at[0], hidden_out.at[0])
    for tick in range(1, ticks):
        start_all(stash_copies(tick))
        send_edge(2 * tick + 1)
        send_edge(2 * tick)
    all_pieces(relay, 1)
    all_pieces(relay, 0)
    for tick in range(ticks):
        ahead, behind = (2 * tick, 2 * tick + 1)
        stage_adjoint(tick)
        if tick == 0:
            wait_all(loads[3])
        over_chunks(units, unit_chunk, call(adjoint_products, tick))
        if tick:
            all_pieces(relay, ahead)
        over_chunks(width, width_chunk, call(back_products, behind))
        all_pieces(start_piece, behind)
        send_out(delta_swap.at[tick], delta_out.at[tick])
        stage_forward(tick)

        def beside_forward(index, tick=tick, behind=behind):
            if turned and tick == 0:
                turn_part(down_dir, down_dir_turned, index)
            if index == 0:
                all_pieces(reduce_in_chip, behind)

        over_chunks(units, unit_chunk, forward_products, beside_forward)
        over_chunks(width, width_chunk, call(down_products, ahead))
        all_pieces(start_piece, ahead)
        finish_backward(tick)
        if tick + 1 < ticks:
            relay_stash(tick + 1)
            stage_stash(tick + 1)

            def beside_next(index, ahead=ahead):
                if index == 0:
                    all_pieces(reduce_in_chip, ahead)

            over_chunks(units, unit_chunk, call(stash_products, tick + 1), beside_next)
            send_out(hid_swap.at[tick + 1], hidden_out.at[tick + 1])
            finish_forward(tick)
            all_pieces(relay, behind + 2)
        else:
            all_pieces(reduce_in_chip, ahead)
            finish_forward(tick)

    for lane in range(2 * ticks):

        def sent(lane=lane):
            for piece in range(pieces):
                for copy in shift_copies(lane, piece):
                    copy.wait_send()

        def sent_edge(lane=lane):
            for copy in edge_copies(lane):
                copy.wait_send()

        pl.when(sends(lane))(sent)
        pl.when(at_edge(lane))(sent_edge)
        for piece in range(pieces):
            relay_copy(lane, piece).wait_send()
            core_copy(lane, piece).wait_send()
            for copy in chip_copies(lane, piece):
                copy.wait_send()
    for tick in range(ticks):
        for copy in stash_copies(tick):
            copy.wait_send()
        stash_relay_copy(tick).wait_send()
    for copy in outs:
        copy.wait()


def curvature_kernel(
    stash_hbm, delta_hbm, hidden_hbm, adj_hbm, final_hbm,
    act, act_tan, adj_new, adj_new_tan, up_hbm, down_hbm,
    stash_sw, delta_sw, hidden_sw, adj, final, up_out, down_out, in_sems, row_sems, up_sems, down_sems,
):
    sources = (stash_hbm, delta_hbm, hidden_hbm, adj_hbm, final_hbm)
    targets = (stash_sw, delta_sw, hidden_sw, adj, final)
    loads = [
        pltpu.make_async_copy(source, target, in_sems.at[i])
        for i, (source, target) in enumerate(zip(sources, targets))
    ]
    for load in loads:
        load.start()
    for load in loads:
        load.wait()
    row_copies = [
        pltpu.make_async_copy(final.at[i], target.at[0], row_sems.at[i])
        for i, target in enumerate((act, act_tan, adj_new, adj_new_tan))
    ]
    for copy in row_copies:
        copy.start()

    def product(left, right, out, target, sems):
        chunk = out.shape[0] // sems.shape[0]

        def part(piece):
            where = pl.ds(piece * chunk, chunk)
            if not isinstance(piece, int):
                where = pl.ds(pl.multiple_of(piece * chunk, chunk), chunk)
            out[where, :] = product_first(left[:, where], right[...]).astype(bf16)
            copy = pltpu.make_async_copy(out.at[where, :], target.at[0, where, :], sems.at[piece])
            copy.start()

        return part

    up_part = product(stash_sw, delta_sw, up_out, up_hbm, up_sems)
    down_part = product(hidden_sw, adj, down_out, down_hbm, down_sems)
    if up_sems.shape[0] == down_sems.shape[0] > 1:

        def step(piece, carry):
            up_part(piece)
            down_part(piece)
            return carry

        lax.fori_loop(0, up_sems.shape[0], step, 0)
    else:
        for piece in range(up_sems.shape[0]):
            up_part(piece)
        for piece in range(down_sems.shape[0]):
            down_part(piece)
    for out, target, sems in ((up_out, up_hbm, up_sems), (down_out, down_hbm, down_sems)):
        chunk = out.shape[0] // sems.shape[0]
        for piece in range(sems.shape[0]):
            where = pl.ds(piece * chunk, chunk)
            pltpu.make_async_copy(out.at[where, :], target.at[0, where, :], sems.at[piece]).wait()
    for copy in row_copies:
        copy.wait()


def shards(
    carry_act, carry_act_tan, carry_adj, carry_adj_tan, fresh_act, loss_cot, stash_act,
    stash_act_tan, norm_gain, up_weight, down_weight, up_dir, down_dir,
):
    sections, n_dp = (lax.axis_size("section"), lax.axis_size("dp"))
    chips = n_dp // 2
    ticks, rows, width = fresh_act.shape
    units = up_weight.shape[2]
    band = n_dp * 2 * rows
    tall = 2 * band
    pieces = width // lane_chunk(width, 768)
    lanes = 2 * ticks
    vmem, anywhere = (
        pl.BlockSpec(memory_space=pltpu.VMEM),
        pl.BlockSpec(memory_space=pl.ANY),
    )
    block = (2 * rows, width)
    turned = units % 128 == 0
    up_turn, down_turn = ((units, width), (width, units)) if turned else ((16, 128), (16, 128))
    stash_out, adj_out, hidden_out, delta_out, final_out = pl.pallas_call(
        functools.partial(relay_kernel, sections, n_dp, ticks),
        out_shape=(
            jax.ShapeDtypeStruct((ticks, 2, chips) + block, bf16),
            jax.ShapeDtypeStruct((ticks, 2, chips) + block, bf16),
            jax.ShapeDtypeStruct((ticks, band, units), bf16),
            jax.ShapeDtypeStruct((ticks, band, units), bf16),
            jax.ShapeDtypeStruct((4, rows, width), bf16),
        ),
        in_specs=[anywhere] * 13,
        out_specs=(anywhere,) * 4 + (vmem,),
        scratch_shapes=[
            pltpu.VMEM((width, units), bf16),
            pltpu.VMEM((units, width), bf16),
            pltpu.VMEM((width, units), bf16),
            pltpu.VMEM((units, width), bf16),
            pltpu.VMEM(up_turn, bf16),
            pltpu.VMEM(down_turn, bf16),
            pltpu.VMEM(up_turn, bf16),
            pltpu.VMEM(down_turn, bf16),
            pltpu.VMEM((1, width), bf16),
            pltpu.VMEM((ticks,) + block, bf16),
            pltpu.VMEM((tall, width), bf16),
            pltpu.VMEM((tall, width), bf16),
            pltpu.VMEM((band, units), bf16),
            pltpu.VMEM((band, units), bf16),
            pltpu.VMEM((ticks, n_dp, rows, units), f32),
            pltpu.VMEM((ticks, n_dp, rows, units), f32),
            pltpu.VMEM((ticks, band, units), bf16),
            pltpu.VMEM((band, units), bf16),
            pltpu.VMEM((band, units), bf16),
            pltpu.VMEM((ticks, band, units), bf16),
            pltpu.VMEM((band, width), bf16),
            pltpu.VMEM((ticks, 2, chips) + block, bf16),
            pltpu.VMEM((lanes, 2, chips) + block, bf16),
            pltpu.VMEM((lanes,) + block, bf16),
            pltpu.VMEM((lanes, 2, chips) + block, bf16),
            pltpu.VMEM((lanes, chips) + block, bf16),
            pltpu.VMEM((lanes, chips - 1) + block, bf16),
            pltpu.VMEM((lanes, chips - 1) + block, bf16),
            pltpu.SemaphoreType.DMA((4, 3)),
            pltpu.SemaphoreType.DMA((ticks + 3, 2)),
            pltpu.SemaphoreType.DMA((lanes,)),
            pltpu.SemaphoreType.DMA((4 * ticks,)),
            pltpu.SemaphoreType.DMA((lanes, pieces, 2)),
            pltpu.SemaphoreType.DMA((lanes, pieces, 2, chips - 1)),
            pltpu.SemaphoreType.DMA((lanes, pieces, 2, chips)),
            pltpu.SemaphoreType.DMA((lanes, 2, chips)),
            pltpu.SemaphoreType.DMA((lanes, pieces, 2)),
            pltpu.SemaphoreType.DMA((ticks, 2, chips)),
            pltpu.SemaphoreType.DMA((ticks, 2)),
        ],
        compiler_params=pltpu.CompilerParams(
            collective_id=0, has_side_effects=True, vmem_limit_bytes=60 * 1024 * 1024
        ),
        name="relay",
    )(
        carry_act, carry_act_tan, carry_adj, carry_adj_tan, fresh_act, loss_cot, stash_act,
        stash_act_tan, norm_gain, up_weight, down_weight, up_dir, down_dir,
    )
    deep = band * ticks
    stash_sw = stash_out.reshape(deep, width)
    delta_sw = delta_out.reshape(deep, units)
    hidden_sw = hidden_out.reshape(deep, units)
    adj_flat = adj_out.reshape(deep, width)
    rows_shape = jax.ShapeDtypeStruct((1, rows, width), bf16)
    return tuple(
        pl.pallas_call(
            curvature_kernel,
            out_shape=(rows_shape,) * 4
            + (
                jax.ShapeDtypeStruct((1, width, units), bf16),
                jax.ShapeDtypeStruct((1, units, width), bf16),
            ),
            in_specs=[anywhere] * 5,
            out_specs=(anywhere,) * 6,
            scratch_shapes=[
                pltpu.VMEM((deep, width), bf16),
                pltpu.VMEM((deep, units), bf16),
                pltpu.VMEM((deep, units), bf16),
                pltpu.VMEM((deep, width), bf16),
                pltpu.VMEM((4, rows, width), bf16),
                pltpu.VMEM((width, units), bf16),
                pltpu.VMEM((units, width), bf16),
                pltpu.SemaphoreType.DMA((5,)),
                pltpu.SemaphoreType.DMA((4,)),
                pltpu.SemaphoreType.DMA((width // lane_chunk(width, 768),)),
                pltpu.SemaphoreType.DMA((units // lane_chunk(units, 384),)),
            ],
            compiler_params=pltpu.CompilerParams(vmem_limit_bytes=60 * 1024 * 1024),
            name="curvature",
        )(stash_sw, delta_sw, hidden_sw, adj_flat, final_out)
    )


def solution(mesh):
    in_specs = (
        P("section", "dp", None),
        P("section", "dp", None),
        P("section", "dp", None),
        P("section", "dp", None),
        P(None, "dp", None),
        P(None, "dp", None),
        P("section", None, "dp", None),
        P("section", None, "dp", None),
        P("section", None),
        P("section", None, "dp"),
        P("section", "dp", None),
        P("section", None, "dp"),
        P("section", "dp", None),
    )
    out_specs = (
        P("section", "dp", None),
        P("section", "dp", None),
        P("section", "dp", None),
        P("section", "dp", None),
        P("section", None, "dp"),
        P("section", "dp", None),
    )
    return jax.shard_map(shards, mesh=mesh, in_specs=in_specs, out_specs=out_specs, check_vma=False)
```

```python
import functools

import jax
import jax.numpy as jnp
from jax import lax
from jax.experimental import pallas as pl
from jax.experimental.pallas import tpu as pltpu
from jax.sharding import PartitionSpec as P

sqrt_two_over_pi = 0.7978845608028654
cubic_coef = 0.044715
norm_eps = 1e-06


def gelu_parts(linear):
    inner_arg = sqrt_two_over_pi * (linear + cubic_coef * linear * linear * linear)
    first_slope = sqrt_two_over_pi * (1.0 + 3.0 * cubic_coef * linear * linear)
    second_slope = 6.0 * sqrt_two_over_pi * cubic_coef * linear
    tanh_value = jnp.tanh(inner_arg)
    sech_square = 1.0 - tanh_value * tanh_value
    gelu_value = 0.5 * linear * (1.0 + tanh_value)
    gelu_first = 0.5 * (1.0 + tanh_value) + 0.5 * linear * sech_square * first_slope
    gelu_second = sech_square * (
        first_slope - linear * tanh_value * first_slope * first_slope + 0.5 * linear * second_slope
    )
    return (gelu_value, gelu_first, gelu_second)


def matrix_product(left, right):
    return jnp.dot(left, right, preferred_element_type=jnp.float32)


def product_last(left, right):
    return lax.dot_general(
        left, right, (((1,), (1,)), ((), ())), preferred_element_type=jnp.float32
    )


def product_first(left, right):
    return lax.dot_general(
        left, right, (((0,), (0,)), ((), ())), preferred_element_type=jnp.float32
    )


f32, bf16 = (jnp.float32, jnp.bfloat16)
MESH = pl.DeviceIdType.MESH


def lane_chunk(size, wanted):
    fits = [c for c in range(128, wanted + 1, 128) if size % c == 0]
    return max(fits) if fits else size


def over_chunks(size, chunk, body, after=None):
    for index in range(size // chunk):
        body(pl.ds(index * chunk, chunk))
        if after is not None:
            after(index)


def turn(source, target, chunk):
    def step(index, carry):
        where = pl.ds(pl.multiple_of(index * chunk, chunk), chunk)
        target[:, where] = source[where, :].T
        return carry

    lax.fori_loop(0, source.shape[0] // chunk, step, 0)


def pair(value, tangent):
    blocks, rows, width = value.shape
    return jnp.stack([value, tangent], axis=1).reshape(blocks * 2 * rows, width)


def unpair(stacked, rows):
    wide = stacked.astype(f32).reshape(-1, 2, rows, stacked.shape[-1])
    return (wide[:, 0], wide[:, 1])


def norm_pair(stacked, gain, rows):
    values, values_tan = unpair(stacked, rows)
    inverse = lax.rsqrt(jnp.mean(values * values, axis=-1, keepdims=True) + norm_eps)
    inverse_tan = -(inverse * inverse * inverse) * jnp.mean(
        values * values_tan, axis=-1, keepdims=True
    )
    return (values * inverse * gain, (values_tan * inverse + values * inverse_tan) * gain)


def relay_kernel(
    sections, n_dp, ticks,
    carry_act, carry_act_tan, carry_adj, carry_adj_tan, fresh_act, loss_cot, stash_act,
    stash_act_tan, norm_gain, up_hbm, down_hbm, up_dir_hbm, down_dir_hbm,
    final_out, curve_up, curve_down,
    up, down, up_dir, down_dir, up_dir_turned, down_dir_turned,
    gain_row, own_stash,
    left, left_dir, hid, hid_dir, slope, bend, hid_swap, delta, delta_dir, delta_swap,
    adj_dir, stash_all, gathered, outgoing, partial, from_core, to_chip, from_chip,
    weight_sems, small_sems, edge_loads, core_sems, chip_sems, shift_sems, edge_sems,
    relay_sems, stash_sems, stash_relay,
):
    chips = n_dp // 2
    rows = carry_act.shape[1]
    width = carry_act.shape[2]
    units = up.shape[1]
    band = n_dp * 2 * rows
    unit_chunk = lane_chunk(units, 384)
    width_chunk = lane_chunk(width, 768)
    pieces = width // width_chunk
    section, part = (lax.axis_index("section"), lax.axis_index("dp"))
    chip, core = (part // 2, part % 2)
    other = 1 - core
    partner = (section, chip * 2 + other)
    first, last_one = (section == 0, section == sections - 1)
    inner_first, inner_last = (section > 0, section < sections - 1)
    turned = units % 128 == 0
    up_turned, down_turned = (curve_down, curve_up)

    def chip_at(step):
        return lax.rem(chip + step, chips)

    def load_pair(index, value, tangent, target):
        return [
            pltpu.make_async_copy(value, target.at[pl.ds(0, rows)], small_sems.at[index, 0]),
            pltpu.make_async_copy(tangent, target.at[pl.ds(rows, rows)], small_sems.at[index, 1]),
        ]

    stash_loads = [
        load_pair(t, stash_act.at[0, t], stash_act_tan.at[0, t], own_stash.at[t])
        for t in range(ticks)
    ]
    adj_loads = load_pair(ticks, carry_adj.at[0], carry_adj_tan.at[0], outgoing.at[1])
    act_loads = load_pair(ticks + 1, carry_act.at[0], carry_act_tan.at[0], outgoing.at[0])
    gain_load = pltpu.make_async_copy(norm_gain, gain_row, small_sems.at[ticks + 2, 0])

    def edge_load(lane):
        source = (fresh_act, loss_cot)[lane % 2]
        return pltpu.make_async_copy(
            source.at[lane // 2],
            gathered.at[lane, core, chip, pl.ds(0, rows)],
            edge_loads.at[lane],
        )

    def at_edge(lane):
        return first if lane % 2 == 0 else last_one

    def inside(lane):
        return inner_first if lane % 2 == 0 else inner_last

    def sends(lane):
        return inner_last if lane % 2 == 0 else inner_first

    def call(work, *given):
        return functools.partial(work, *given)

    def start_all(copies):
        for copy in copies:
            copy.start()

    def wait_all(copies):
        for copy in copies:
            copy.wait()

    gain_load.start()
    for tick in range(ticks):
        start_all(stash_loads[tick])
    start_all(adj_loads)
    start_all(act_loads)
    for lane in range(2 * ticks):
        pl.when(at_edge(lane))(edge_load(lane).start)

    def weight_loads(number, source, target):
        cuts = weight_sems.shape[1]
        part = target.shape[0] // cuts
        return [
            pltpu.make_async_copy(
                source.at[0, pl.ds(cut * part, part)],
                target.at[pl.ds(cut * part, part)],
                weight_sems.at[number, cut],
            )
            for cut in range(cuts)
        ]

    loads = [
        weight_loads(i, source, target)
        for i, (source, target) in enumerate(
            ((up_hbm, up), (up_dir_hbm, up_dir), (down_hbm, down), (down_dir_hbm, down_dir))
        )
    ]

    barrier = pltpu.get_barrier_semaphore()

    def greet(where, place):
        pl.semaphore_signal(barrier, inc=1, device_id=(where, place), device_id_type=MESH)

    def greet_section(where):
        for step in range(chips):
            greet(where, chip_at(step) * 2 + core)

    pl.when(inner_last)(lambda: greet_section(section + 1))
    pl.when(inner_first)(lambda: greet_section(section - 1))
    pl.semaphore_signal(barrier, inc=1, device_id=partner, device_id_type=MESH)
    for step in range(1, chips):
        greet(section, chip_at(step) * 2 + core)

    def columns(piece):
        if isinstance(piece, int):
            return pl.ds(piece * width_chunk, width_chunk)
        return pl.ds(pl.multiple_of(piece * width_chunk, width_chunk), width_chunk)

    def shift_copies(lane, piece):
        where = section + 1 if lane % 2 == 0 else section - 1
        cols = columns(piece)
        return [
            pltpu.make_async_remote_copy(
                src_ref=outgoing.at[lane, :, cols],
                dst_ref=gathered.at[lane, core, chip, :, cols],
                send_sem=shift_sems.at[lane, piece, 0, step],
                recv_sem=shift_sems.at[lane, piece, 1, step],
                device_id=(where, chip_at(step) * 2 + core),
                device_id_type=MESH,
            )
            for step in range(chips)
        ]

    def edge_copies(lane):
        return [
            pltpu.make_async_remote_copy(
                src_ref=gathered.at[lane, core, chip],
                dst_ref=gathered.at[lane, core, chip],
                send_sem=edge_sems.at[lane, 0, step],
                recv_sem=edge_sems.at[lane, 1, step],
                device_id=(section, chip_at(step) * 2 + core),
                device_id_type=MESH,
            )
            for step in range(1, chips)
        ]

    def relay_copy(lane, piece):
        cols = columns(piece)
        return pltpu.make_async_remote_copy(
            src_ref=gathered.at[lane, core, :, :, cols],
            dst_ref=gathered.at[lane, core, :, :, cols],
            send_sem=relay_sems.at[lane, piece, 0],
            recv_sem=relay_sems.at[lane, piece, 1],
            device_id=partner,
            device_id_type=MESH,
        )

    def stash_copies(tick):
        return [
            pltpu.make_async_remote_copy(
                src_ref=stash_all.at[tick, core, chip],
                dst_ref=stash_all.at[tick, core, chip],
                send_sem=stash_sems.at[tick, 0, step],
                recv_sem=stash_sems.at[tick, 1, step],
                device_id=(section, chip_at(step) * 2 + core),
                device_id_type=MESH,
            )
            for step in range(1, chips)
        ]

    def stash_relay_copy(tick):
        return pltpu.make_async_remote_copy(
            src_ref=stash_all.at[tick, core],
            dst_ref=stash_all.at[tick, core],
            send_sem=stash_relay.at[tick, 0],
            recv_sem=stash_relay.at[tick, 1],
            device_id=partner,
            device_id_type=MESH,
        )

    def relay_stash(tick):
        for copy in stash_copies(tick):
            copy.wait_recv()
        stash_relay_copy(tick).start()

    def core_copy(lane, piece):
        return pltpu.make_async_remote_copy(
            src_ref=partial.at[lane, other, :, :, columns(piece)],
            dst_ref=from_core.at[lane, :, :, columns(piece)],
            send_sem=core_sems.at[lane, piece, 0],
            recv_sem=core_sems.at[lane, piece, 1],
            device_id=partner,
            device_id_type=MESH,
        )

    def chip_copies(lane, piece):
        return [
            pltpu.make_async_remote_copy(
                src_ref=to_chip.at[lane, step - 1, :, columns(piece)],
                dst_ref=from_chip.at[lane, step - 1, :, columns(piece)],
                send_sem=chip_sems.at[lane, piece, 0, step - 1],
                recv_sem=chip_sems.at[lane, piece, 1, step - 1],
                device_id=(section, chip_at(step) * 2 + core),
                device_id_type=MESH,
            )
            for step in range(1, chips)
        ]

    def shift(lane, piece):
        pl.when(sends(lane))(lambda: start_all(shift_copies(lane, piece)))

    def relay(lane, piece):
        def from_section():
            for copy in shift_copies(lane, piece):
                copy.wait_recv()

        def from_edge():
            for copy in edge_copies(lane):
                copy.wait_recv()

        pl.when(inside(lane))(from_section)
        if piece == 0:
            pl.when(at_edge(lane))(from_edge)
        relay_copy(lane, piece).start()

    def reduce_in_chip(lane, piece):
        core_copy(lane, piece).wait_recv()
        cols = columns(piece)
        for step in range(1, chips):
            place = chip_at(step)
            summed = partial[lane, core, place, :, cols].astype(f32)
            summed = summed + from_core[lane, place, :, cols].astype(f32)
            to_chip[lane, step - 1, :, cols] = summed.astype(bf16)
        start_all(chip_copies(lane, piece))

    def reduced(lane, piece):
        for copy in chip_copies(lane, piece):
            copy.wait_recv()
        cols = columns(piece)
        total = partial[lane, core, chip, :, cols].astype(f32)
        total = total + from_core[lane, chip, :, cols].astype(f32)
        for step in range(chips - 1):
            total = total + from_chip[lane, step, :, cols].astype(f32)
        return total

    def norm_stash(tick):
        gain = gain_row[...].astype(f32)
        normed, normed_tan = norm_pair(own_stash[tick], gain, rows)
        stash_all[tick, core, chip] = pair(normed, normed_tan).astype(bf16)

    def stage_forward(tick):
        lane = 2 * tick
        for piece in range(pieces):
            relay_copy(lane, piece).wait_recv()
        gain = gain_row[...].astype(f32)
        for block in range(n_dp):
            where = pl.ds(block * 2 * rows, 2 * rows)
            normed, normed_tan = norm_pair(
                gathered[lane, block // chips, block % chips], gain, rows
            )
            left[where, :] = pair(normed, normed_tan).astype(bf16)
            left_dir[where, :] = pair(jnp.zeros_like(normed), normed).astype(bf16)

    def stage_stash(tick):
        stash_relay_copy(tick).wait_recv()
        for block in range(n_dp):
            where = pl.ds(band + block * 2 * rows, 2 * rows)
            stacked = stash_all[tick, block // chips, block % chips]
            left[where, :] = stacked
            value = unpair(stacked, rows)[0]
            left_dir[where, :] = pair(jnp.zeros_like(value), value).astype(bf16)

    def forward_products(cols):
        stacked = matrix_product(left[:band, :], up[:, cols]) + matrix_product(
            left_dir[:band, :], up_dir[:, cols]
        )
        linear, linear_tan = unpair(stacked, rows)
        value, slope_now, _ = gelu_parts(linear)
        hid[:, cols] = pair(value, slope_now * linear_tan).astype(bf16)
        hid_dir[:, cols] = pair(jnp.zeros_like(value), value).astype(bf16)

    def stash_products(tick, cols):
        stacked = matrix_product(left[band:, :], up[:, cols]) + matrix_product(
            left_dir[band:, :], up_dir[:, cols]
        )
        linear, linear_tan = unpair(stacked, rows)
        value, slope_now, second = gelu_parts(linear)
        hid_swap[tick, :, cols] = pair(slope_now * linear_tan, value).astype(bf16)
        slope[tick, :, :, cols] = slope_now
        bend[tick, :, :, cols] = second * linear_tan

    def down_products(lane, cols):
        stacked = matrix_product(hid[...], down[:, cols]) + matrix_product(
            hid_dir[...], down_dir[:, cols]
        )
        partial[lane, :, :, :, cols] = stacked.astype(bf16).reshape(2, chips, 2 * rows, -1)

    def adjoint_products(tick, cols):
        adjoint = gathered[2 * tick + 1].reshape(band, width)
        if turned and tick:
            stacked = matrix_product(adjoint, down_turned[:, cols]) + matrix_product(
                adj_dir[...], down_dir_turned[:, cols]
            )
        elif turned:
            stacked = matrix_product(adjoint, down_turned[:, cols]) + product_last(
                adj_dir[...], down_dir[cols, :]
            )
        else:
            stacked = product_last(adjoint, down[cols, :]) + product_last(
                adj_dir[...], down_dir[cols, :]
            )
        upstream, upstream_tan = unpair(stacked, rows)
        slope_now, second_tan = (slope[tick, :, :, cols], bend[tick, :, :, cols])
        value = upstream * slope_now
        tangent = upstream_tan * slope_now + upstream * second_tan
        delta[:, cols] = pair(value, tangent).astype(bf16)
        delta_dir[:, cols] = pair(jnp.zeros_like(value), value).astype(bf16)
        delta_swap[tick, :, cols] = pair(tangent, value).astype(bf16)

    def back_products(lane, cols):
        if turned:
            stacked = matrix_product(delta[...], up_turned[:, cols]) + matrix_product(
                delta_dir[...], up_dir_turned[:, cols]
            )
        else:
            stacked = product_last(delta[...], up[cols, :]) + product_last(
                delta_dir[...], up_dir[cols, :]
            )
        partial[lane, :, :, :, cols] = stacked.astype(bf16).reshape(2, chips, 2 * rows, -1)

    def finish_forward(tick):
        lane = 2 * tick
        for piece in range(pieces):
            cols = columns(piece)
            total = reduced(lane, piece) + gathered[lane, core, chip, :, cols].astype(f32)
            if tick + 1 < ticks:
                outgoing[lane + 2, :, cols] = total.astype(bf16)
                shift(lane + 2, piece)
            else:
                final_out[0, :, cols] = total[:rows].astype(bf16)
                final_out[1, :, cols] = total[rows:].astype(bf16)

    def finish_backward(tick):
        lane = 2 * tick + 1
        total = jnp.concatenate([reduced(lane, piece) for piece in range(pieces)], axis=-1)
        summed, summed_tan = (total[:rows], total[rows:])
        gain = gain_row[...].astype(f32)
        arriving = gathered[lane, core, chip].astype(f32)
        both = own_stash[tick].astype(f32)
        values, values_tan = (both[:rows], both[rows:])
        inverse = lax.rsqrt(jnp.mean(values * values, axis=-1, keepdims=True) + norm_eps)
        cube = inverse * inverse * inverse
        inverse_tan = -cube * jnp.mean(values * values_tan, axis=-1, keepdims=True)
        weighted, weighted_tan = (summed * gain, summed_tan * gain)
        moment = jnp.mean(values * weighted, axis=-1, keepdims=True)
        moment_tan = jnp.mean(
            values_tan * weighted + values * weighted_tan, axis=-1, keepdims=True
        )
        value = arriving[:rows] + inverse * weighted - cube * values * moment
        tangent = (
            arriving[rows:]
            + inverse_tan * weighted
            + inverse * weighted_tan
            - 3.0 * inverse * inverse * inverse_tan * values * moment
            - cube * values_tan * moment
            - cube * values * moment_tan
        )
        if tick + 1 < ticks:
            outgoing[lane + 2] = pair(value[None], tangent[None]).astype(bf16)
            for piece in range(pieces):
                shift(lane + 2, piece)
        else:
            final_out[2] = value.astype(bf16)
            final_out[3] = tangent.astype(bf16)

    def start_piece(lane, piece):
        core_copy(lane, piece).start()

    def stage_adjoint(tick):
        lane = 2 * tick + 1
        for piece in range(pieces):
            relay_copy(lane, piece).wait_recv()
        for block in range(n_dp):
            value = unpair(gathered[lane, block // chips, block % chips], rows)[0]
            adj_dir[pl.ds(block * 2 * rows, 2 * rows), :] = pair(
                jnp.zeros_like(value), value
            ).astype(bf16)

    def enter_edge(lane):
        def load_rows():
            edge_load(lane).wait()
            gathered[lane, core, chip, rows:, :] = jnp.zeros((rows, width), bf16)

        pl.when(at_edge(lane))(load_rows)

    def send_edge(lane):
        pl.when(at_edge(lane))(lambda: start_all(edge_copies(lane)))

    gain_load.wait()
    for tick in range(ticks):
        wait_all(stash_loads[tick])
    wait_all(adj_loads)
    wait_all(act_loads)
    for lane in range(2 * ticks):
        enter_edge(lane)
    for load in loads:
        start_all(load)
    norm_stash(0)
    sides = inner_first.astype(jnp.int32) + inner_last.astype(jnp.int32)
    pl.semaphore_wait(barrier, chips + chips * sides)
    start_all(stash_copies(0))

    def first_shift(lane):
        copies = [shift_copies(lane, piece) for piece in range(pieces)]
        for step in range(chips):
            for piece in range(pieces):
                copies[piece][step].start()

    pl.when(sends(1))(call(first_shift, 1))
    send_edge(1)
    for tick in range(1, ticks):
        norm_stash(tick)

    def curvature():
        deep = ticks * band

        adjoints = jnp.concatenate(
            [gathered[2 * tick + 1].reshape(band, width) for tick in range(ticks)], axis=0
        )
        deltas = delta_swap[...].reshape(deep, units)
        for index in range(max(pieces, units // unit_chunk)):
            if index < pieces:
                where = columns(index)
                curve_up[where, :] = product_first(
                    stash_all[:, :, :, :, where].reshape(deep, width_chunk), deltas
                ).astype(bf16)
            if index < units // unit_chunk:
                where = pl.ds(index * unit_chunk, unit_chunk)
                curve_down[where, :] = product_first(
                    hid_swap[:, :, where].reshape(deep, unit_chunk), adjoints
                ).astype(bf16)

    def turn_part(source, target, index):
        where = pl.ds(index * unit_chunk, unit_chunk)
        target[:, where] = source[where, :].T

    def all_pieces(work, *given):
        for piece in range(pieces):
            work(*given, piece)

    def enter_weights(number, source, target):
        part = source.shape[0] // len(loads[number])
        for cut, load in enumerate(loads[number]):
            load.wait()
            if turned:
                where = pl.ds(cut * part, part)
                target[:, where] = source[where, :].T

    enter_weights(0, up, up_turned)
    relay_stash(0)
    enter_weights(1, up_dir, up_dir_turned)
    stage_stash(0)
    pl.when(sends(0))(call(first_shift, 0))
    send_edge(0)
    wait_all(loads[2])

    def beside_stash(index):
        if turned:
            turn_part(down, down_turned, index)

    over_chunks(units, unit_chunk, call(stash_products, 0), beside_stash)
    for tick in range(1, ticks):
        start_all(stash_copies(tick))
        send_edge(2 * tick + 1)
        send_edge(2 * tick)
    all_pieces(relay, 1)
    for tick in range(ticks):
        ahead, behind = (2 * tick, 2 * tick + 1)
        stage_adjoint(tick)
        if tick == 0:
            wait_all(loads[3])
        over_chunks(units, unit_chunk, call(adjoint_products, tick))
        all_pieces(relay, ahead)
        over_chunks(width, width_chunk, call(back_products, behind))
        all_pieces(start_piece, behind)
        if tick + 1 < ticks:
            relay_stash(tick + 1)
        stage_forward(tick)

        def beside_forward(index, tick=tick, behind=behind):
            if turned and tick == 0:
                turn_part(down_dir, down_dir_turned, index)
            if index == 0:
                all_pieces(reduce_in_chip, behind)

        over_chunks(units, unit_chunk, forward_products, beside_forward)
        over_chunks(width, width_chunk, call(down_products, ahead))
        all_pieces(start_piece, ahead)
        finish_backward(tick)
        if tick + 1 < ticks:
            stage_stash(tick + 1)

            def beside_next(index, ahead=ahead):
                if index == 0:
                    all_pieces(reduce_in_chip, ahead)

            over_chunks(units, unit_chunk, call(stash_products, tick + 1), beside_next)
            finish_forward(tick)
            all_pieces(relay, behind + 2)
        else:
            all_pieces(reduce_in_chip, ahead)
            curvature()
            finish_forward(tick)

    for lane in range(2 * ticks):

        def sent(lane=lane):
            for piece in range(pieces):
                for copy in shift_copies(lane, piece):
                    copy.wait_send()

        def sent_edge(lane=lane):
            for copy in edge_copies(lane):
                copy.wait_send()

        pl.when(sends(lane))(sent)
        pl.when(at_edge(lane))(sent_edge)
        for piece in range(pieces):
            relay_copy(lane, piece).wait_send()
            core_copy(lane, piece).wait_send()
            for copy in chip_copies(lane, piece):
                copy.wait_send()
    for tick in range(ticks):
        for copy in stash_copies(tick):
            copy.wait_send()
        stash_relay_copy(tick).wait_send()


def deliver_kernel(
    final, curve_up, curve_down, act, act_tan, adj_new, adj_new_tan, up_hbm, down_hbm, row_sems, part_sems
):
    copies = []
    for number, (source, target) in enumerate(((curve_up, up_hbm), (curve_down, down_hbm))):
        cuts = part_sems.shape[1]
        part = source.shape[0] // cuts
        for cut in range(cuts):
            where = pl.ds(cut * part, part)
            copies.append(
                pltpu.make_async_copy(
                    source.at[where], target.at[0, where], part_sems.at[number, cut]
                )
            )
    for i, target in enumerate((act, act_tan, adj_new, adj_new_tan)):
        copies.append(pltpu.make_async_copy(final.at[i], target.at[0], row_sems.at[i]))
    for copy in copies:
        copy.start()
    for copy in copies:
        copy.wait()


def shards(
    carry_act, carry_act_tan, carry_adj, carry_adj_tan, fresh_act, loss_cot, stash_act,
    stash_act_tan, norm_gain, up_weight, down_weight, up_dir, down_dir,
):
    sections, n_dp = (lax.axis_size("section"), lax.axis_size("dp"))
    chips = n_dp // 2
    ticks, rows, width = fresh_act.shape
    units = up_weight.shape[2]
    band = n_dp * 2 * rows
    tall = 2 * band
    pieces = width // lane_chunk(width, 768)
    lanes = 2 * ticks
    vmem, anywhere = (
        pl.BlockSpec(memory_space=pltpu.VMEM),
        pl.BlockSpec(memory_space=pl.ANY),
    )
    block = (2 * rows, width)
    turned = units % 128 == 0
    up_turn, down_turn = ((units, width), (width, units)) if turned else ((16, 128), (16, 128))
    final_out, curve_up, curve_down = pl.pallas_call(
        functools.partial(relay_kernel, sections, n_dp, ticks),
        out_shape=(
            pltpu.VMEM((4, rows, width), bf16),
            pltpu.VMEM((width, units), bf16),
            pltpu.VMEM((units, width), bf16),
        ),
        in_specs=[anywhere] * 13,
        out_specs=(vmem,) * 3,
        scratch_shapes=[
            pltpu.VMEM((width, units), bf16),
            pltpu.VMEM((units, width), bf16),
            pltpu.VMEM((width, units), bf16),
            pltpu.VMEM((units, width), bf16),
            pltpu.VMEM(up_turn, bf16),
            pltpu.VMEM(down_turn, bf16),
            pltpu.VMEM((1, width), bf16),
            pltpu.VMEM((ticks,) + block, bf16),
            pltpu.VMEM((tall, width), bf16),
            pltpu.VMEM((tall, width), bf16),
            pltpu.VMEM((band, units), bf16),
            pltpu.VMEM((band, units), bf16),
            pltpu.VMEM((ticks, n_dp, rows, units), f32),
            pltpu.VMEM((ticks, n_dp, rows, units), f32),
            pltpu.VMEM((ticks, band, units), bf16),
            pltpu.VMEM((band, units), bf16),
            pltpu.VMEM((band, units), bf16),
            pltpu.VMEM((ticks, band, units), bf16),
            pltpu.VMEM((band, width), bf16),
            pltpu.VMEM((ticks, 2, chips) + block, bf16),
            pltpu.VMEM((lanes, 2, chips) + block, bf16),
            pltpu.VMEM((lanes,) + block, bf16),
            pltpu.VMEM((lanes, 2, chips) + block, bf16),
            pltpu.VMEM((lanes, chips) + block, bf16),
            pltpu.VMEM((lanes, chips - 1) + block, bf16),
            pltpu.VMEM((lanes, chips - 1) + block, bf16),
            pltpu.SemaphoreType.DMA((4, 3)),
            pltpu.SemaphoreType.DMA((ticks + 3, 2)),
            pltpu.SemaphoreType.DMA((lanes,)),
            pltpu.SemaphoreType.DMA((lanes, pieces, 2)),
            pltpu.SemaphoreType.DMA((lanes, pieces, 2, chips - 1)),
            pltpu.SemaphoreType.DMA((lanes, pieces, 2, chips)),
            pltpu.SemaphoreType.DMA((lanes, 2, chips)),
            pltpu.SemaphoreType.DMA((lanes, pieces, 2)),
            pltpu.SemaphoreType.DMA((ticks, 2, chips)),
            pltpu.SemaphoreType.DMA((ticks, 2)),
        ],
        compiler_params=pltpu.CompilerParams(
            collective_id=0, has_side_effects=True, vmem_limit_bytes=46 * 1024 * 1024
        ),
        name="relay",
    )(
        carry_act, carry_act_tan, carry_adj, carry_adj_tan, fresh_act, loss_cot, stash_act,
        stash_act_tan, norm_gain, up_weight, down_weight, up_dir, down_dir,
    )
    rows_shape = jax.ShapeDtypeStruct((1, rows, width), bf16)
    return tuple(
        pl.pallas_call(
            deliver_kernel,
            out_shape=(rows_shape,) * 4
            + (
                jax.ShapeDtypeStruct((1, width, units), bf16),
                jax.ShapeDtypeStruct((1, units, width), bf16),
            ),
            in_specs=[vmem] * 3,
            out_specs=(anywhere,) * 6,
            scratch_shapes=[
                pltpu.SemaphoreType.DMA((4,)),
                pltpu.SemaphoreType.DMA((2, 3)),
            ],
            compiler_params=pltpu.CompilerParams(vmem_limit_bytes=1024 * 1024),
            name="deliver",
        )(final_out, curve_up, curve_down)
    )


def solution(mesh):
    in_specs = (
        P("section", "dp", None),
        P("section", "dp", None),
        P("section", "dp", None),
        P("section", "dp", None),
        P(None, "dp", None),
        P(None, "dp", None),
        P("section", None, "dp", None),
        P("section", None, "dp", None),
        P("section", None),
        P("section", None, "dp"),
        P("section", "dp", None),
        P("section", None, "dp"),
        P("section", "dp", None),
    )
    out_specs = (
        P("section", "dp", None),
        P("section", "dp", None),
        P("section", "dp", None),
        P("section", "dp", None),
        P("section", None, "dp"),
        P("section", "dp", None),
    )
    return jax.shard_map(shards, mesh=mesh, in_specs=in_specs, out_specs=out_specs, check_vma=False)
```

```python
import functools

import jax
import jax.numpy as jnp
from jax import lax
from jax.experimental import pallas as pl
from jax.experimental.pallas import tpu as pltpu
from jax.sharding import PartitionSpec as P

sqrt_two_over_pi = 0.7978845608028654
cubic_coef = 0.044715
norm_eps = 1e-06


def gelu_parts(linear):
    inner_arg = sqrt_two_over_pi * (linear + cubic_coef * linear * linear * linear)
    first_slope = sqrt_two_over_pi * (1.0 + 3.0 * cubic_coef * linear * linear)
    second_slope = 6.0 * sqrt_two_over_pi * cubic_coef * linear
    tanh_value = jnp.tanh(inner_arg)
    sech_square = 1.0 - tanh_value * tanh_value
    gelu_value = 0.5 * linear * (1.0 + tanh_value)
    gelu_first = 0.5 * (1.0 + tanh_value) + 0.5 * linear * sech_square * first_slope
    gelu_second = sech_square * (
        first_slope - linear * tanh_value * first_slope * first_slope + 0.5 * linear * second_slope
    )
    return (gelu_value, gelu_first, gelu_second)


def matrix_product(left, right):
    return jnp.dot(left, right, preferred_element_type=jnp.float32)


def product_last(left, right):
    return lax.dot_general(
        left, right, (((1,), (1,)), ((), ())), preferred_element_type=jnp.float32
    )


def product_first(left, right):
    return lax.dot_general(
        left, right, (((0,), (0,)), ((), ())), preferred_element_type=jnp.float32
    )


f32, bf16 = (jnp.float32, jnp.bfloat16)
MESH = pl.DeviceIdType.MESH


def lane_chunk(size, wanted):
    fits = [c for c in range(128, wanted + 1, 128) if size % c == 0]
    return max(fits) if fits else size


def over_chunks(size, chunk, body, after=None):
    for index in range(size // chunk):
        body(pl.ds(index * chunk, chunk))
        if after is not None:
            after(index)


def turn(source, target, chunk):
    def step(index, carry):
        where = pl.ds(pl.multiple_of(index * chunk, chunk), chunk)
        target[:, where] = source[where, :].T
        return carry

    lax.fori_loop(0, source.shape[0] // chunk, step, 0)


def pair(value, tangent):
    blocks, rows, width = value.shape
    return jnp.stack([value, tangent], axis=1).reshape(blocks * 2 * rows, width)


def unpair(stacked, rows):
    wide = stacked.astype(f32).reshape(-1, 2, rows, stacked.shape[-1])
    return (wide[:, 0], wide[:, 1])


def norm_pair(stacked, gain, rows):
    values, values_tan = unpair(stacked, rows)
    inverse = lax.rsqrt(jnp.mean(values * values, axis=-1, keepdims=True) + norm_eps)
    inverse_tan = -(inverse * inverse * inverse) * jnp.mean(
        values * values_tan, axis=-1, keepdims=True
    )
    return (values * inverse * gain, (values_tan * inverse + values * inverse_tan) * gain)


def relay_kernel(
    sections, n_dp, ticks,
    carry_act, carry_act_tan, carry_adj, carry_adj_tan, fresh_act, loss_cot, stash_act,
    stash_act_tan, norm_gain, up_hbm, down_hbm, up_dir_hbm, down_dir_hbm,
    final_out, curve_up, curve_down,
    up, down, up_dir, down_dir, up_dir_turned, down_dir_turned,
    gain_row, own_stash,
    left, left_dir, hid, hid_dir, slope, bend, hid_swap, delta, delta_dir, delta_swap,
    adj_dir, stash_all, gathered, outgoing, partial, from_core, to_chip, from_chip,
    weight_sems, small_sems, edge_loads, core_sems, chip_sems, shift_sems, edge_sems,
    relay_sems, stash_sems, stash_relay,
):
    chips = n_dp // 2
    rows = carry_act.shape[1]
    width = carry_act.shape[2]
    units = up.shape[1]
    band = n_dp * 2 * rows
    unit_chunk = lane_chunk(units, 384)
    width_chunk = lane_chunk(width, 768)
    pieces = width // width_chunk
    section, part = (lax.axis_index("section"), lax.axis_index("dp"))
    chip, core = (part // 2, part % 2)
    other = 1 - core
    partner = (section, chip * 2 + other)
    first, last_one = (section == 0, section == sections - 1)
    inner_first, inner_last = (section > 0, section < sections - 1)
    turned = units % 128 == 0
    up_turned, down_turned = (curve_down, curve_up)

    def chip_at(step):
        return lax.rem(chip + step, chips)

    def load_pair(index, value, tangent, target):
        return [
            pltpu.make_async_copy(value, target.at[pl.ds(0, rows)], small_sems.at[index, 0]),
            pltpu.make_async_copy(tangent, target.at[pl.ds(rows, rows)], small_sems.at[index, 1]),
        ]

    stash_loads = [
        load_pair(t, stash_act.at[0, t], stash_act_tan.at[0, t], own_stash.at[t])
        for t in range(ticks)
    ]
    adj_loads = load_pair(ticks, carry_adj.at[0], carry_adj_tan.at[0], outgoing.at[1])
    act_loads = load_pair(ticks + 1, carry_act.at[0], carry_act_tan.at[0], outgoing.at[0])
    gain_load = pltpu.make_async_copy(norm_gain, gain_row, small_sems.at[ticks + 2, 0])

    def edge_load(lane):
        source = (fresh_act, loss_cot)[lane % 2]
        return pltpu.make_async_copy(
            source.at[lane // 2],
            gathered.at[lane, core, chip, pl.ds(0, rows)],
            edge_loads.at[lane],
        )

    def at_edge(lane):
        return first if lane % 2 == 0 else last_one

    def inside(lane):
        return inner_first if lane % 2 == 0 else inner_last

    def sends(lane):
        return inner_last if lane % 2 == 0 else inner_first

    def call(work, *given):
        return functools.partial(work, *given)

    def start_all(copies):
        for copy in copies:
            copy.start()

    def wait_all(copies):
        for copy in copies:
            copy.wait()

    gain_load.start()
    for tick in range(ticks):
        start_all(stash_loads[tick])
    start_all(adj_loads)
    start_all(act_loads)
    for lane in range(2 * ticks):
        pl.when(at_edge(lane))(edge_load(lane).start)

    def weight_loads(number, source, target):
        cuts = weight_sems.shape[1]
        part = target.shape[0] // cuts
        return [
            pltpu.make_async_copy(
                source.at[0, pl.ds(cut * part, part)],
                target.at[pl.ds(cut * part, part)],
                weight_sems.at[number, cut],
            )
            for cut in range(cuts)
        ]

    loads = [
        weight_loads(i, source, target)
        for i, (source, target) in enumerate(
            ((up_hbm, up), (up_dir_hbm, up_dir), (down_hbm, down), (down_dir_hbm, down_dir))
        )
    ]

    barrier = pltpu.get_barrier_semaphore()

    def greet(where, place):
        pl.semaphore_signal(barrier, inc=1, device_id=(where, place), device_id_type=MESH)

    def greet_section(where):
        for step in range(chips):
            greet(where, chip_at(step) * 2 + core)

    pl.when(inner_last)(lambda: greet_section(section + 1))
    pl.when(inner_first)(lambda: greet_section(section - 1))
    pl.semaphore_signal(barrier, inc=1, device_id=partner, device_id_type=MESH)
    for step in range(1, chips):
        greet(section, chip_at(step) * 2 + core)

    def columns(piece):
        if isinstance(piece, int):
            return pl.ds(piece * width_chunk, width_chunk)
        return pl.ds(pl.multiple_of(piece * width_chunk, width_chunk), width_chunk)

    def shift_copies(lane, piece):
        where = section + 1 if lane % 2 == 0 else section - 1
        cols = columns(piece)
        return [
            pltpu.make_async_remote_copy(
                src_ref=outgoing.at[lane, :, cols],
                dst_ref=gathered.at[lane, core, chip, :, cols],
                send_sem=shift_sems.at[lane, piece, 0, step],
                recv_sem=shift_sems.at[lane, piece, 1, step],
                device_id=(where, chip_at(step) * 2 + core),
                device_id_type=MESH,
            )
            for step in range(chips)
        ]

    def edge_copies(lane):
        return [
            pltpu.make_async_remote_copy(
                src_ref=gathered.at[lane, core, chip],
                dst_ref=gathered.at[lane, core, chip],
                send_sem=edge_sems.at[lane, 0, step],
                recv_sem=edge_sems.at[lane, 1, step],
                device_id=(section, chip_at(step) * 2 + core),
                device_id_type=MESH,
            )
            for step in range(1, chips)
        ]

    def relay_copy(lane, piece):
        cols = columns(piece)
        return pltpu.make_async_remote_copy(
            src_ref=gathered.at[lane, core, :, :, cols],
            dst_ref=gathered.at[lane, core, :, :, cols],
            send_sem=relay_sems.at[lane, piece, 0],
            recv_sem=relay_sems.at[lane, piece, 1],
            device_id=partner,
            device_id_type=MESH,
        )

    def stash_copies(tick):
        return [
            pltpu.make_async_remote_copy(
                src_ref=stash_all.at[tick, core, chip],
                dst_ref=stash_all.at[tick, core, chip],
                send_sem=stash_sems.at[tick, 0, step],
                recv_sem=stash_sems.at[tick, 1, step],
                device_id=(section, chip_at(step) * 2 + core),
                device_id_type=MESH,
            )
            for step in range(1, chips)
        ]

    def stash_relay_copy(tick):
        return pltpu.make_async_remote_copy(
            src_ref=stash_all.at[tick, core],
            dst_ref=stash_all.at[tick, core],
            send_sem=stash_relay.at[tick, 0],
            recv_sem=stash_relay.at[tick, 1],
            device_id=partner,
            device_id_type=MESH,
        )

    def relay_stash(tick):
        for copy in stash_copies(tick):
            copy.wait_recv()
        stash_relay_copy(tick).start()

    def core_copy(lane, piece):
        return pltpu.make_async_remote_copy(
            src_ref=partial.at[lane, other, :, :, columns(piece)],
            dst_ref=from_core.at[lane, :, :, columns(piece)],
            send_sem=core_sems.at[lane, piece, 0],
            recv_sem=core_sems.at[lane, piece, 1],
            device_id=partner,
            device_id_type=MESH,
        )

    def chip_copies(lane, piece):
        return [
            pltpu.make_async_remote_copy(
                src_ref=to_chip.at[lane, step - 1, :, columns(piece)],
                dst_ref=from_chip.at[lane, step - 1, :, columns(piece)],
                send_sem=chip_sems.at[lane, piece, 0, step - 1],
                recv_sem=chip_sems.at[lane, piece, 1, step - 1],
                device_id=(section, chip_at(step) * 2 + core),
                device_id_type=MESH,
            )
            for step in range(1, chips)
        ]

    def shift(lane, piece):
        pl.when(sends(lane))(lambda: start_all(shift_copies(lane, piece)))

    def relay(lane, piece):
        def from_section():
            for copy in shift_copies(lane, piece):
                copy.wait_recv()

        def from_edge():
            for copy in edge_copies(lane):
                copy.wait_recv()

        pl.when(inside(lane))(from_section)
        if piece == 0:
            pl.when(at_edge(lane))(from_edge)
        relay_copy(lane, piece).start()

    def reduce_in_chip(lane, piece):
        core_copy(lane, piece).wait_recv()
        cols = columns(piece)
        for step in range(1, chips):
            place = chip_at(step)
            summed = partial[lane, core, place, :, cols].astype(f32)
            summed = summed + from_core[lane, place, :, cols].astype(f32)
            to_chip[lane, step - 1, :, cols] = summed.astype(bf16)
        start_all(chip_copies(lane, piece))

    def reduced(lane, piece):
        for copy in chip_copies(lane, piece):
            copy.wait_recv()
        cols = columns(piece)
        total = partial[lane, core, chip, :, cols].astype(f32)
        total = total + from_core[lane, chip, :, cols].astype(f32)
        for step in range(chips - 1):
            total = total + from_chip[lane, step, :, cols].astype(f32)
        return total

    def norm_stash(tick):
        gain = gain_row[...].astype(f32)
        normed, normed_tan = norm_pair(own_stash[tick], gain, rows)
        stash_all[tick, core, chip] = pair(normed, normed_tan).astype(bf16)

    def stage_forward(tick):
        lane = 2 * tick
        for piece in range(pieces):
            relay_copy(lane, piece).wait_recv()
        gain = gain_row[...].astype(f32)
        for block in range(n_dp):
            where = pl.ds(block * 2 * rows, 2 * rows)
            normed, normed_tan = norm_pair(
                gathered[lane, block // chips, block % chips], gain, rows
            )
            left[where, :] = pair(normed, normed_tan).astype(bf16)
            left_dir[where, :] = pair(jnp.zeros_like(normed), normed).astype(bf16)

    def stage_stash(tick):
        stash_relay_copy(tick).wait_recv()
        for block in range(n_dp):
            where = pl.ds(band + block * 2 * rows, 2 * rows)
            stacked = stash_all[tick, block // chips, block % chips]
            left[where, :] = stacked
            value = unpair(stacked, rows)[0]
            left_dir[where, :] = pair(jnp.zeros_like(value), value).astype(bf16)

    def forward_products(cols):
        stacked = matrix_product(left[:band, :], up[:, cols]) + matrix_product(
            left_dir[:band, :], up_dir[:, cols]
        )
        linear, linear_tan = unpair(stacked, rows)
        value, slope_now, _ = gelu_parts(linear)
        hid[:, cols] = pair(value, slope_now * linear_tan).astype(bf16)
        hid_dir[:, cols] = pair(jnp.zeros_like(value), value).astype(bf16)

    def stash_products(tick, cols):
        stacked = matrix_product(left[band:, :], up[:, cols]) + matrix_product(
            left_dir[band:, :], up_dir[:, cols]
        )
        linear, linear_tan = unpair(stacked, rows)
        value, slope_now, second = gelu_parts(linear)
        hid_swap[tick, :, cols] = pair(slope_now * linear_tan, value).astype(bf16)
        slope[tick, :, :, cols] = slope_now
        bend[tick, :, :, cols] = second * linear_tan

    def down_products(lane, cols):
        stacked = matrix_product(hid[...], down[:, cols]) + matrix_product(
            hid_dir[...], down_dir[:, cols]
        )
        partial[lane, :, :, :, cols] = stacked.astype(bf16).reshape(2, chips, 2 * rows, -1)

    def adjoint_products(tick, cols):
        adjoint = gathered[2 * tick + 1].reshape(band, width)
        if turned and tick:
            stacked = matrix_product(adjoint, down_turned[:, cols]) + matrix_product(
                adj_dir[...], down_dir_turned[:, cols]
            )
        elif turned:
            stacked = matrix_product(adjoint, down_turned[:, cols]) + product_last(
                adj_dir[...], down_dir[cols, :]
            )
        else:
            stacked = product_last(adjoint, down[cols, :]) + product_last(
                adj_dir[...], down_dir[cols, :]
            )
        upstream, upstream_tan = unpair(stacked, rows)
        slope_now, second_tan = (slope[tick, :, :, cols], bend[tick, :, :, cols])
        value = upstream * slope_now
        tangent = upstream_tan * slope_now + upstream * second_tan
        delta[:, cols] = pair(value, tangent).astype(bf16)
        delta_dir[:, cols] = pair(jnp.zeros_like(value), value).astype(bf16)
        delta_swap[tick, :, cols] = pair(tangent, value).astype(bf16)

    def back_products(lane, cols):
        if turned:
            stacked = matrix_product(delta[...], up_turned[:, cols]) + matrix_product(
                delta_dir[...], up_dir_turned[:, cols]
            )
        else:
            stacked = product_last(delta[...], up[cols, :]) + product_last(
                delta_dir[...], up_dir[cols, :]
            )
        partial[lane, :, :, :, cols] = stacked.astype(bf16).reshape(2, chips, 2 * rows, -1)

    def finish_forward(tick):
        lane = 2 * tick
        for piece in range(pieces):
            cols = columns(piece)
            total = reduced(lane, piece) + gathered[lane, core, chip, :, cols].astype(f32)
            if tick + 1 < ticks:
                outgoing[lane + 2, :, cols] = total.astype(bf16)
                shift(lane + 2, piece)
            else:
                final_out[0, :, cols] = total[:rows].astype(bf16)
                final_out[1, :, cols] = total[rows:].astype(bf16)

    def finish_backward(tick):
        lane = 2 * tick + 1
        total = jnp.concatenate([reduced(lane, piece) for piece in range(pieces)], axis=-1)
        summed, summed_tan = (total[:rows], total[rows:])
        gain = gain_row[...].astype(f32)
        arriving = gathered[lane, core, chip].astype(f32)
        both = own_stash[tick].astype(f32)
        values, values_tan = (both[:rows], both[rows:])
        inverse = lax.rsqrt(jnp.mean(values * values, axis=-1, keepdims=True) + norm_eps)
        cube = inverse * inverse * inverse
        inverse_tan = -cube * jnp.mean(values * values_tan, axis=-1, keepdims=True)
        weighted, weighted_tan = (summed * gain, summed_tan * gain)
        moment = jnp.mean(values * weighted, axis=-1, keepdims=True)
        moment_tan = jnp.mean(
            values_tan * weighted + values * weighted_tan, axis=-1, keepdims=True
        )
        value = arriving[:rows] + inverse * weighted - cube * values * moment
        tangent = (
            arriving[rows:]
            + inverse_tan * weighted
            + inverse * weighted_tan
            - 3.0 * inverse * inverse * inverse_tan * values * moment
            - cube * values_tan * moment
            - cube * values * moment_tan
        )
        if tick + 1 < ticks:
            outgoing[lane + 2] = pair(value[None], tangent[None]).astype(bf16)
            for piece in range(pieces):
                shift(lane + 2, piece)
        else:
            final_out[2] = value.astype(bf16)
            final_out[3] = tangent.astype(bf16)

    def start_piece(lane, piece):
        core_copy(lane, piece).start()

    def stage_adjoint(tick):
        lane = 2 * tick + 1
        for piece in range(pieces):
            relay_copy(lane, piece).wait_recv()
        for block in range(n_dp):
            value = unpair(gathered[lane, block // chips, block % chips], rows)[0]
            adj_dir[pl.ds(block * 2 * rows, 2 * rows), :] = pair(
                jnp.zeros_like(value), value
            ).astype(bf16)

    def enter_edge(lane):
        def load_rows():
            edge_load(lane).wait()
            gathered[lane, core, chip, rows:, :] = jnp.zeros((rows, width), bf16)

        pl.when(at_edge(lane))(load_rows)

    def send_edge(lane):
        pl.when(at_edge(lane))(lambda: start_all(edge_copies(lane)))

    gain_load.wait()
    for tick in range(ticks):
        wait_all(stash_loads[tick])
    wait_all(adj_loads)
    wait_all(act_loads)
    for lane in range(2 * ticks):
        enter_edge(lane)
    for load in loads:
        start_all(load)
    norm_stash(0)
    sides = inner_first.astype(jnp.int32) + inner_last.astype(jnp.int32)
    pl.semaphore_wait(barrier, chips + chips * sides)
    start_all(stash_copies(0))

    def first_shift(lane):
        copies = [shift_copies(lane, piece) for piece in range(pieces)]
        for step in range(chips):
            for piece in range(pieces):
                copies[piece][step].start()

    pl.when(sends(1))(call(first_shift, 1))
    send_edge(1)
    for tick in range(1, ticks):
        norm_stash(tick)

    def curvature():
        deep = ticks * band

        adjoints = jnp.concatenate(
            [gathered[2 * tick + 1].reshape(band, width) for tick in range(ticks)], axis=0
        )
        deltas = delta_swap[...].reshape(deep, units)
        for index in range(max(pieces, units // unit_chunk)):
            if index < pieces:
                where = columns(index)
                curve_up[where, :] = product_first(
                    stash_all[:, :, :, :, where].reshape(deep, width_chunk), deltas
                ).astype(bf16)
            if index < units // unit_chunk:
                where = pl.ds(index * unit_chunk, unit_chunk)
                curve_down[where, :] = product_first(
                    hid_swap[:, :, where].reshape(deep, unit_chunk), adjoints
                ).astype(bf16)

    def turn_part(source, target, index):
        where = pl.ds(index * unit_chunk, unit_chunk)
        target[:, where] = source[where, :].T

    def all_pieces(work, *given):
        for piece in range(pieces):
            work(*given, piece)

    def enter_weights(number, source, target):
        part = source.shape[0] // len(loads[number])
        for cut, load in enumerate(loads[number]):
            load.wait()
            if turned:
                where = pl.ds(cut * part, part)
                target[:, where] = source[where, :].T

    enter_weights(0, up, up_turned)
    enter_weights(1, up_dir, up_dir_turned)
    relay_stash(0)
    stage_stash(0)
    pl.when(sends(0))(call(first_shift, 0))
    send_edge(0)
    wait_all(loads[2])

    parts = units // unit_chunk

    def beside_stash(index):
        if turned:
            turn_part(down, down_turned, index)
        if index == max(parts - 2, 0):
            all_pieces(relay, 1)

    over_chunks(units, unit_chunk, call(stash_products, 0), beside_stash)
    for tick in range(1, ticks):
        start_all(stash_copies(tick))
        send_edge(2 * tick + 1)
        send_edge(2 * tick)
    for tick in range(ticks):
        ahead, behind = (2 * tick, 2 * tick + 1)
        stage_adjoint(tick)
        if tick == 0:
            wait_all(loads[3])
        over_chunks(units, unit_chunk, call(adjoint_products, tick))
        all_pieces(relay, ahead)
        over_chunks(width, width, call(back_products, behind))
        all_pieces(start_piece, behind)
        if tick + 1 < ticks:
            relay_stash(tick + 1)
        stage_forward(tick)

        def beside_forward(index, tick=tick, behind=behind):
            reduce_at = 0 if tick + 1 < ticks else min(1, parts - 1)
            if turned and tick == 0:
                turn_part(down_dir, down_dir_turned, index)
            if index == reduce_at:
                all_pieces(reduce_in_chip, behind)

        over_chunks(units, unit_chunk, forward_products, beside_forward)
        over_chunks(width, width, call(down_products, ahead))
        all_pieces(start_piece, ahead)
        if tick + 1 < ticks:
            finish_backward(tick)
            stage_stash(tick + 1)

            def beside_next(index, ahead=ahead):
                if index == min(1, parts - 1):
                    all_pieces(reduce_in_chip, ahead)

            over_chunks(units, unit_chunk, call(stash_products, tick + 1), beside_next)
            finish_forward(tick)
            all_pieces(relay, behind + 2)
        else:
            all_pieces(reduce_in_chip, ahead)
            finish_backward(tick)
            curvature()
            finish_forward(tick)

    for lane in range(2 * ticks):

        def sent(lane=lane):
            for piece in range(pieces):
                for copy in shift_copies(lane, piece):
                    copy.wait_send()

        def sent_edge(lane=lane):
            for copy in edge_copies(lane):
                copy.wait_send()

        pl.when(sends(lane))(sent)
        pl.when(at_edge(lane))(sent_edge)
        for piece in range(pieces):
            relay_copy(lane, piece).wait_send()
            core_copy(lane, piece).wait_send()
            for copy in chip_copies(lane, piece):
                copy.wait_send()
    for tick in range(ticks):
        for copy in stash_copies(tick):
            copy.wait_send()
        stash_relay_copy(tick).wait_send()


def deliver_kernel(
    final, curve_up, curve_down, act, act_tan, adj_new, adj_new_tan, up_hbm, down_hbm, row_sems, part_sems
):
    copies = []
    for number, (source, target) in enumerate(((curve_up, up_hbm), (curve_down, down_hbm))):
        cuts = part_sems.shape[1]
        part = source.shape[0] // cuts
        for cut in range(cuts):
            where = pl.ds(cut * part, part)
            copies.append(
                pltpu.make_async_copy(
                    source.at[where], target.at[0, where], part_sems.at[number, cut]
                )
            )
    for i, target in enumerate((act, act_tan, adj_new, adj_new_tan)):
        copies.append(pltpu.make_async_copy(final.at[i], target.at[0], row_sems.at[i]))
    for copy in copies:
        copy.start()
    for copy in copies:
        copy.wait()


def shards(
    carry_act, carry_act_tan, carry_adj, carry_adj_tan, fresh_act, loss_cot, stash_act,
    stash_act_tan, norm_gain, up_weight, down_weight, up_dir, down_dir,
):
    sections, n_dp = (lax.axis_size("section"), lax.axis_size("dp"))
    chips = n_dp // 2
    ticks, rows, width = fresh_act.shape
    units = up_weight.shape[2]
    band = n_dp * 2 * rows
    tall = 2 * band
    pieces = width // lane_chunk(width, 768)
    lanes = 2 * ticks
    vmem, anywhere = (
        pl.BlockSpec(memory_space=pltpu.VMEM),
        pl.BlockSpec(memory_space=pl.ANY),
    )
    block = (2 * rows, width)
    turned = units % 128 == 0
    up_turn, down_turn = ((units, width), (width, units)) if turned else ((16, 128), (16, 128))
    final_out, curve_up, curve_down = pl.pallas_call(
        functools.partial(relay_kernel, sections, n_dp, ticks),
        out_shape=(
            pltpu.VMEM((4, rows, width), bf16),
            pltpu.VMEM((width, units), bf16),
            pltpu.VMEM((units, width), bf16),
        ),
        in_specs=[anywhere] * 13,
        out_specs=(vmem,) * 3,
        scratch_shapes=[
            pltpu.VMEM((width, units), bf16),
            pltpu.VMEM((units, width), bf16),
            pltpu.VMEM((width, units), bf16),
            pltpu.VMEM((units, width), bf16),
            pltpu.VMEM(up_turn, bf16),
            pltpu.VMEM(down_turn, bf16),
            pltpu.VMEM((1, width), bf16),
            pltpu.VMEM((ticks,) + block, bf16),
            pltpu.VMEM((tall, width), bf16),
            pltpu.VMEM((tall, width), bf16),
            pltpu.VMEM((band, units), bf16),
            pltpu.VMEM((band, units), bf16),
            pltpu.VMEM((ticks, n_dp, rows, units), f32),
            pltpu.VMEM((ticks, n_dp, rows, units), f32),
            pltpu.VMEM((ticks, band, units), bf16),
            pltpu.VMEM((band, units), bf16),
            pltpu.VMEM((band, units), bf16),
            pltpu.VMEM((ticks, band, units), bf16),
            pltpu.VMEM((band, width), bf16),
            pltpu.VMEM((ticks, 2, chips) + block, bf16),
            pltpu.VMEM((lanes, 2, chips) + block, bf16),
            pltpu.VMEM((lanes,) + block, bf16),
            pltpu.VMEM((lanes, 2, chips) + block, bf16),
            pltpu.VMEM((lanes, chips) + block, bf16),
            pltpu.VMEM((lanes, chips - 1) + block, bf16),
            pltpu.VMEM((lanes, chips - 1) + block, bf16),
            pltpu.SemaphoreType.DMA((4, 3)),
            pltpu.SemaphoreType.DMA((ticks + 3, 2)),
            pltpu.SemaphoreType.DMA((lanes,)),
            pltpu.SemaphoreType.DMA((lanes, pieces, 2)),
            pltpu.SemaphoreType.DMA((lanes, pieces, 2, chips - 1)),
            pltpu.SemaphoreType.DMA((lanes, pieces, 2, chips)),
            pltpu.SemaphoreType.DMA((lanes, 2, chips)),
            pltpu.SemaphoreType.DMA((lanes, pieces, 2)),
            pltpu.SemaphoreType.DMA((ticks, 2, chips)),
            pltpu.SemaphoreType.DMA((ticks, 2)),
        ],
        compiler_params=pltpu.CompilerParams(
            collective_id=0, has_side_effects=True, vmem_limit_bytes=46 * 1024 * 1024
        ),
        name="relay",
    )(
        carry_act, carry_act_tan, carry_adj, carry_adj_tan, fresh_act, loss_cot, stash_act,
        stash_act_tan, norm_gain, up_weight, down_weight, up_dir, down_dir,
    )
    rows_shape = jax.ShapeDtypeStruct((1, rows, width), bf16)
    return tuple(
        pl.pallas_call(
            deliver_kernel,
            out_shape=(rows_shape,) * 4
            + (
                jax.ShapeDtypeStruct((1, width, units), bf16),
                jax.ShapeDtypeStruct((1, units, width), bf16),
            ),
            in_specs=[vmem] * 3,
            out_specs=(anywhere,) * 6,
            scratch_shapes=[
                pltpu.SemaphoreType.DMA((4,)),
                pltpu.SemaphoreType.DMA((2, 3)),
            ],
            compiler_params=pltpu.CompilerParams(vmem_limit_bytes=1024 * 1024),
            name="deliver",
        )(final_out, curve_up, curve_down)
    )


def solution(mesh):
    in_specs = (
        P("section", "dp", None),
        P("section", "dp", None),
        P("section", "dp", None),
        P("section", "dp", None),
        P(None, "dp", None),
        P(None, "dp", None),
        P("section", None, "dp", None),
        P("section", None, "dp", None),
        P("section", None),
        P("section", None, "dp"),
        P("section", "dp", None),
        P("section", None, "dp"),
        P("section", "dp", None),
    )
    out_specs = (
        P("section", "dp", None),
        P("section", "dp", None),
        P("section", "dp", None),
        P("section", "dp", None),
        P("section", None, "dp"),
        P("section", "dp", None),
    )
    return jax.shard_map(shards, mesh=mesh, in_specs=in_specs, out_specs=out_specs, check_vma=False)
```
